32 devices in a mesh: data: 1 (over z), tensor: 32 (over y, x, core).
Axes of the slice: x: 4, y: 4, z: 1, core: 2. Of those that a mesh axis runs over, the one named last changes fastest.
The devices are a block of a 4x4x8 slice.
Arguments:
- token_ids: int32 [8192], P(('data', 'tensor'))
- emb_table: bfloat16 [384, 1472], P('tensor')
- norm_gain: bfloat16 [1472], replicated
- w_up: bfloat16 [1472, 3584], P(None, 'tensor')
- w_down: bfloat16 [3584, 1472], P('tensor')
- grad_out: bfloat16 [8192, 1472], P(('data', 'tensor'))
Outputs:
- output 1: bfloat16 [8192, 1472], P(('data', 'tensor'))
- output 2: float32 [384, 1472], P(('data', 'tensor'))
- output 3: float32 [1472, 3584], P('data', 'tensor')
- output 4: float32 [3584, 1472], P(('data', 'tensor'))
All inputs are finite; a program needn't handle non-finite values.
Results may differ from the reference program's by a relative error of at most 0.00926022.
Values are sent between devices in bfloat16 or wider.
A program may use at most 768 MiB of HBM per device.

```python
import math
import jax
import jax.numpy as jnp
from jax import lax

VOCAB_SIZE = 384
MODEL_DIM = 1472
FFN_DIM = 3584
TOKENS = 8192
HOT_IDS = 64
EPS = 1e-6
ROW_BLOCK = math.gcd(TOKENS, 2048)
NUM_BLOCKS = TOKENS // ROW_BLOCK


def draw_ids(key):
    key_uni, key_table, key_pick, key_coin = jax.random.split(key, 4)
    uniform_ids = jax.random.randint(key_uni, (TOKENS,), 0, VOCAB_SIZE)
    hot_table = jax.random.randint(key_table, (HOT_IDS,), 0, VOCAB_SIZE)
    hot_ids = hot_table[jax.random.randint(key_pick, (TOKENS,), 0, HOT_IDS)]
    coin_flip = jax.random.randint(key_coin, (TOKENS,), 0, 2)
    token_ids = jnp.where(coin_flip == 0, uniform_ids, hot_ids)
    token_ids = token_ids.at[0].set(0).at[TOKENS - 1].set(VOCAB_SIZE - 1)
    return token_ids.astype(jnp.int32)


def setup_inputs(seed: int = 0, part: int = 0) -> dict:
    shared_key, part_root = jax.random.split(jax.random.key(seed))
    key_emb, key_gain, key_up, key_down = jax.random.split(shared_key, 4)
    key_ids, key_grad = jax.random.split(jax.random.fold_in(part_root, part))
    emb_table = jax.random.normal(key_emb, (VOCAB_SIZE, MODEL_DIM), jnp.float32)
    norm_gain = 1.0 + 0.4 * jax.random.normal(key_gain, (MODEL_DIM,), jnp.float32)
    w_up = jax.random.normal(key_up, (MODEL_DIM, FFN_DIM), jnp.float32) * MODEL_DIM ** -0.5
    w_down = jax.random.normal(key_down, (FFN_DIM, MODEL_DIM), jnp.float32) * FFN_DIM ** -0.5
    grad_out = jax.random.normal(key_grad, (TOKENS, MODEL_DIM), jnp.float32)
    return {
        'token_ids': draw_ids(key_ids),
        'emb_table': emb_table.astype(jnp.bfloat16),
        'norm_gain': norm_gain.astype(jnp.bfloat16),
        'w_up': w_up.astype(jnp.bfloat16),
        'w_down': w_down.astype(jnp.bfloat16),
        'grad_out': grad_out.astype(jnp.bfloat16),
    }


def rms_norm(x_rows, gain_f):
    inv_rms = lax.rsqrt(jnp.mean(x_rows * x_rows, axis=-1, keepdims=True) + EPS)
    return x_rows * inv_rms * gain_f


def gelu_tanh(values):
    return jax.nn.gelu(values, approximate=True)


def reference(token_ids, emb_table, norm_gain, w_up, w_down, grad_out):
    gain_f = norm_gain.astype(jnp.float32)
    x_rows = jnp.take(emb_table, token_ids, axis=0)
    x_blocks = x_rows.reshape(NUM_BLOCKS, ROW_BLOCK, MODEL_DIM)
    grad_blocks = grad_out.reshape(NUM_BLOCKS, ROW_BLOCK, MODEL_DIM)

    def block_step(acc_pair, block_in):
        acc_up, acc_down = acc_pair
        x_blk = block_in[0].astype(jnp.float32)
        grad_blk = block_in[1]
        normed_f, norm_back = jax.vjp(lambda x_in: rms_norm(x_in, gain_f), x_blk)
        normed = normed_f.astype(jnp.bfloat16)
        pre_act = jnp.dot(normed, w_up, preferred_element_type=jnp.float32).astype(jnp.bfloat16)
        act_f, gelu_back = jax.vjp(gelu_tanh, pre_act.astype(jnp.float32))
        hidden = act_f.astype(jnp.bfloat16)
        y_blk = jnp.dot(hidden, w_down, preferred_element_type=jnp.float32)
        out_blk = (x_blk + y_blk).astype(jnp.bfloat16)
        d_hidden = jnp.dot(grad_blk, w_down.T, preferred_element_type=jnp.float32)
        d_pre = gelu_back(d_hidden)[0].astype(jnp.bfloat16)
        acc_down = acc_down + jnp.dot(hidden.T, grad_blk, preferred_element_type=jnp.float32)
        acc_up = acc_up + jnp.dot(normed.T, d_pre, preferred_element_type=jnp.float32)
        d_norm = jnp.dot(d_pre, w_up.T, preferred_element_type=jnp.float32)
        dx_blk = (grad_blk.astype(jnp.float32) + norm_back(d_norm)[0]).astype(jnp.bfloat16)
        return (acc_up, acc_down), (out_blk, dx_blk)

    zero_acc = (jnp.zeros((MODEL_DIM, FFN_DIM), jnp.float32), jnp.zeros((FFN_DIM, MODEL_DIM), jnp.float32))
    grads, outs = lax.scan(block_step, zero_acc, (x_blocks, grad_blocks))
    out = outs[0].reshape(TOKENS, MODEL_DIM)
    d_x = outs[1].reshape(TOKENS, MODEL_DIM).astype(jnp.float32)
    d_emb = jax.ops.segment_sum(d_x, token_ids, num_segments=VOCAB_SIZE)
    return (out, d_emb, grads[0], grads[1])
```

```python
import functools
import math

import jax
import jax.numpy as jnp
from jax import lax
from jax.experimental import pallas as pl
from jax.experimental.pallas import tpu as pltpu
from jax.sharding import PartitionSpec as P

EPS = 1e-6
BF = jnp.bfloat16
F32 = jnp.float32
CORES = 2
MESH = pl.DeviceIdType.MESH


def gelu_tanh(values):
    return jax.nn.gelu(values, approximate=True)


def parts(v):
    hi = v.astype(BF)
    r = v - hi.astype(F32)
    mid = r.astype(BF)
    lo = (r - mid.astype(F32)).astype(BF)
    return hi, mid, lo


def dot(a, b, ca, cb):
    return lax.dot_general(a, b, (((ca,), (cb,)), ((), ())), preferred_element_type=F32)


def pack(v):
    half = v.shape[1] // 2
    return jnp.concatenate([v[:, :half], v[:, half:]], axis=0).astype(BF)


class Ring:
    def __init__(self, side):
        me = lax.axis_index('tensor')
        self.side = side
        self.core = core = lax.rem(me, CORES)
        self.chip = chip = me // CORES
        x, y = lax.rem(chip, side), chip // side
        self.a = x * (1 - core) + y * core
        self.b = y * (1 - core) + x * core
        self.partner = {'tensor': me + 1 - 2 * core}

    def at(self, da, db):
        a = lax.rem(self.a + da, self.side)
        b = lax.rem(self.b + db, self.side)
        return a * (1 + (self.side - 1) * self.core) + b * (self.side - (self.side - 1) * self.core)

    def dev(self, da, db):
        return {'tensor': self.at(da, db) * CORES + self.core}


PLUS, MINUS = (2, 1), (3, 0)


class Scatter:
    def __init__(self, ring, g, relay, ra, rb, r, ssem, rsem):
        self.ring, self.g, self.relay, self.ra, self.rb, self.r = ring, g, relay, ra, rb, r
        self.ssem, self.rsem = ssem, rsem
        self.sent = []

    def copy(self, src, dst, i, dev):
        return pltpu.make_async_remote_copy(
            src_ref=src, dst_ref=dst, send_sem=self.ssem.at[i], recv_sem=self.rsem.at[i],
            device_id=dev, device_id_type=MESH)

    def c_relay(self, k):
        da = 1 if k in PLUS else 3
        return self.copy(self.g.at[self.ring.at(2, k)], self.relay.at[k], k, self.ring.dev(da, 0))

    def c_ring(self, k, plus):
        da = 1 if plus else 3
        j = 0 if plus else 1
        return self.copy(self.g.at[self.ring.at(da, k)], self.ra.at[j, k], 4 + 4 * j + k, self.ring.dev(da, 0))

    def c_b(self, k):
        return self.copy(self.r.at[k], self.rb.at[k - 1], 11 + k, self.ring.dev(0, k))

    def go(self, c):
        c.start()
        self.sent.append(c)

    def start(self):
        for kp, km in zip(PLUS, MINUS):
            self.go(self.c_relay(kp))
            self.go(self.c_relay(km))
        for kp, km in zip(MINUS, PLUS):
            self.go(self.c_ring(kp, True))
            self.go(self.c_ring(km, False))

    def middle(self):
        for kp, km in zip(PLUS, MINUS):
            for k, plus in ((kp, True), (km, False)):
                self.c_relay(k).wait_recv()
                blk = self.ring.at(1 if plus else 3, k)
                self.g[blk] = self.g[blk] + self.relay[k]
                self.go(self.c_ring(k, plus))

    def short(self):
        for k in (2, 3, 1, 0):
            self.c_ring(k, True).wait_recv()
            self.c_ring(k, False).wait_recv()
            self.r[k] = self.g[self.ring.at(0, k)] + self.ra[0, k] + self.ra[1, k]
            if k:
                self.go(self.c_b(k))

    def finish(self):
        acc = self.r[0]
        for k in (1, 3, 2):
            self.c_b(k).wait_recv()
            acc = acc + self.rb[k - 1]
        return acc

    def drain(self):
        for c in self.sent:
            c.wait_send()


FWD_P, FWD_M = (0, 2), (3, 1)


class Gather:
    def __init__(self, ring, buf, ssem, rsem, dsem, esem):
        self.ring, self.buf = ring, buf
        self.ssem, self.rsem, self.dsem, self.esem = ssem, rsem, dsem, esem
        self.sent = []

    def copy(self, blk, i, dev):
        ref = self.buf.at[self.ring.core, blk]
        return pltpu.make_async_remote_copy(
            src_ref=ref, dst_ref=ref, send_sem=self.ssem.at[i], recv_sem=self.rsem.at[i],
            device_id=dev, device_id_type=MESH)

    def back(self, k):
        return (self.ring.side - k) % self.ring.side

    def go(self, c):
        c.start()
        self.sent.append(c)

    def over(self, blk):
        ref = self.buf.at[self.ring.core, blk]
        c = pltpu.make_async_remote_copy(
            src_ref=ref, dst_ref=ref, send_sem=self.esem.at[blk], recv_sem=self.dsem.at[blk],
            device_id=self.ring.partner, device_id_type=MESH)
        self.go(c)

    def both(self, k):
        blk = self.ring.at(0, self.back(k))
        self.go(self.copy(blk, k, self.ring.dev(1, 0)))
        self.go(self.copy(blk, 4 + k, self.ring.dev(3, 0)))

    def start(self):
        blk = self.ring.at(0, 0)
        for k in (2, 1, 3):
            self.go(self.copy(blk, 11 + k, self.ring.dev(0, k)))
        self.both(0)
        self.over(blk)

    def first(self):
        for k in (1, 3, 2):
            blk = self.ring.at(0, self.back(k))
            self.copy(blk, 11 + k, self.ring.dev(0, k)).wait_recv()
            self.both(k)
            self.over(blk)

    def middle(self):
        for k in (0, 1, 3, 2):
            blk = self.ring.at(3, self.back(k))
            self.copy(blk, k, self.ring.dev(1, 0)).wait_recv()
            if k in FWD_P:
                self.go(self.copy(blk, 8 + k, self.ring.dev(1, 0)))
            self.over(blk)
            blk = self.ring.at(1, self.back(k))
            self.copy(blk, 4 + k, self.ring.dev(3, 0)).wait_recv()
            if k in FWD_M:
                self.go(self.copy(blk, 8 + k, self.ring.dev(3, 0)))
            self.over(blk)

    def last(self):
        for k in (0, 3, 1, 2):
            blk = self.ring.at(2, self.back(k))
            self.copy(blk, 8 + k, self.ring.dev(1, 0)).wait_recv()
            self.over(blk)

    def finish(self):
        n = self.ring.side * self.ring.side
        for blk in range(n):
            ref = self.buf.at[1 - self.ring.core, blk]
            pltpu.make_async_remote_copy(
                src_ref=ref, dst_ref=ref, send_sem=self.esem.at[blk], recv_sem=self.dsem.at[blk],
                device_id=self.ring.partner, device_id_type=MESH).wait_recv()

    def drain(self):
        for c in self.sent:
            c.wait_send()


def kernel(side, ids_in, e_in, g_in, w1_in, w2_in, d_in, out_ref, de_ref, dw1_ref, dw2_ref, s):
    ring = Ring(side)
    core, chip, partner = ring.core, ring.chip, ring.partner
    chips = side * side
    rows_e, width = e_in.shape
    f_loc = w1_in.shape[0]
    half = s['w1p'].shape[2]
    rest = width - half
    rb = s['gs'].shape[1]
    vocab = chips * rb

    def local(src, dst, i):
        return pltpu.make_async_copy(src, dst, s['lsem'].at[i])

    def pair(src, dst, i):
        return pltpu.make_async_remote_copy(
            src_ref=src, dst_ref=dst, send_sem=s['psem'].at[i], recv_sem=s['qsem'].at[i],
            device_id=partner, device_id_type=MESH)

    c_e = local(e_in, s['es'].at[core], 0)
    c_g = local(g_in, s['gsrc'], 1)
    c_i = local(ids_in, s['ids'].at[core], 2)
    c_w1 = local(w1_in, s['w1s'].at[core], 3)
    c_w2 = local(w2_in, s['w2s'].at[core], 4)
    d_own = (local(d_in.at[:half], s['dt'].at[0], 5),
             local(d_in.at[half:], s['dt'].at[0, :rest], 5))
    r_e = pair(e_in, s['es'].at[core], 0)
    r_i = pair(ids_in, s['ids'].at[core], 1)
    r_w1 = pair(w1_in, s['w1s'].at[core], 2)
    r_w2 = pair(w2_in, s['w2s'].at[core], 3)
    d_give = (pair(d_in.at[half:], s['dt'].at[1, :rest], 4),
              pair(d_in.at[:half], s['dt'].at[1], 4))

    for c in (c_e, c_g, c_i):
        c.start()

    @pl.when(core == 1)
    def _():
        for j in range(2):
            s['dt'][j, rest:, :] = jnp.zeros((half - rest, s['dt'].shape[2]), BF)

    barrier = pltpu.get_barrier_semaphore()
    peers = [partner, ring.dev(1, 0), ring.dev(3, 0)] + [ring.dev(0, k) for k in (1, 2, 3)]
    for p in peers:
        pl.semaphore_signal(barrier, inc=1, device_id=p, device_id_type=MESH)
    for i in range(2):
        @pl.when(core == i)
        def _():
            d_own[i].start()
    c_w1.start()
    c_w2.start()
    pl.semaphore_wait(barrier, len(peers))

    r_e.start()
    r_i.start()
    for i in range(2):
        @pl.when(core == i)
        def _():
            d_give[i].start()
    r_w1.start()
    r_w2.start()

    def wide(v):
        return jnp.concatenate([v, jnp.zeros((v.shape[0], 2 * half - width), F32)], axis=1)

    c_e.wait()
    c_g.wait()
    r_e.wait_recv()
    gain = wide(s['gsrc'][...].astype(F32))
    for i in range(2):
        s['e24'][i * rows_e:(i + 1) * rows_e, :] = wide(s['es'][i].astype(F32))

    def inv_rms(x):
        return lax.rsqrt(jnp.sum(x * x, axis=-1, keepdims=True) / width + EPS)

    def mine(v):
        return jnp.where(core == 0, v[:, :half], v[:, half:])

    x24 = s['e24'][...]
    ag_n = Gather(ring, s['bn'], s['nss'], s['nrs'], s['nds'], s['nes'])
    s['bn'][core, chip] = pack(mine(x24 * inv_rms(x24) * gain))
    ag_n.start()

    c_i.wait()
    r_i.wait_recv()
    for i in range(2):
        @pl.when(core == i)
        def _():
            d_own[i].wait()
            d_give[1 - i].wait_recv()

    def hot(ids_row):
        row = lax.broadcasted_iota(jnp.int32, (vocab, ids_row.shape[1]), 0)
        return jnp.where(row == ids_row, 1.0, 0.0).astype(BF)

    tot = dot(hot(s['ids'][core]), s['dt'][0], 1, 1) + dot(hot(s['ids'][1 - core]), s['dt'][1], 1, 1)
    s['gs'][...] = tot.reshape(chips, rb, half)
    rs_s = Scatter(ring, s['gs'], s['lay'].at[0], s['ra'].at[0], s['rb'].at[0], s['r'].at[0], s['ss'].at[0], s['sr'].at[0])
    rs_s.start()

    ag_n.first()

    c_w1.wait()
    c_w2.wait()
    r_w1.wait_recv()
    r_w2.wait_recv()
    for w_src, w_dst in (('w1s', 'w1p'), ('w2s', 'w2p')):
        for i in range(2):
            rows = slice(i * f_loc, (i + 1) * f_loc)
            s[w_dst][0, rows, :] = s[w_src][i, :, :half]
            s[w_dst][1, rows, :] = jnp.concatenate(
                [s[w_src][i, :, half:], jnp.zeros((f_loc, half - rest), BF)], axis=1)

    rs_s.middle()
    ag_n.middle()
    rs_s.short()
    ag_n.last()
    ag_n.finish()

    def unpack(buf, dst):
        q = half // 2
        for h in range(2):
            v = buf[h].astype(F32)
            dst[h, :, :q] = v[:, :rb].reshape(vocab, q).astype(BF)
            dst[h, :, q:] = v[:, rb:].reshape(vocab, q).astype(BF)

    unpack(s['bn'], s['n'])
    pre = (dot(s['n'][0], s['w1p'][0], 1, 1) + dot(s['n'][1], s['w1p'][1], 1, 1)).astype(BF)
    pre_f = pre.astype(F32)
    act, gelu_back = jax.vjp(gelu_tanh, pre_f)
    hid = act.astype(BF)
    s['hid'][...] = hid
    s['slope'][...] = gelu_back(jnp.ones_like(pre_f))[0]
    s['gy'][...] = dot(hid, s['w2p'][core], 1, 0).reshape(chips, rb, half)

    ag_s = Gather(ring, s['bs'], s['sss'], s['srs'], s['sds'], s['ses'])
    s['bs'][core, chip] = rs_s.finish()
    ag_s.start()
    rs_y = Scatter(ring, s['gy'], s['lay'].at[1], s['ra'].at[1], s['rb'].at[1], s['r'].at[1], s['ss'].at[1], s['sr'].at[1])
    rs_y.start()
    ag_s.first()
    ag_s.middle()
    rs_y.middle()
    ag_s.last()
    rs_y.short()
    ag_s.finish()

    def split(i, c):
        v = s['bs'][i].reshape(vocab, half)
        for j, p in enumerate(parts(v)):
            s['sp'][3 * i + j] = p
        return c

    for i in range(2):
        split(i, 0)
    dh = jnp.zeros(s['slope'].shape, F32)
    for j in (2, 1, 0):
        for i in range(2):
            dh = dh + dot(s['sp'][3 * i + j], s['w2p'][i], 1, 1)
    du = dh * s['slope'][...]
    du_p = parts(du)
    dn = jnp.zeros((vocab, half), F32)
    for p in du_p[::-1]:
        dn = dn + dot(p, s['w1p'][core], 1, 0)
    s['gd'][...] = dn.reshape(chips, rb, half)
    rs_d = Scatter(ring, s['gd'], s['lay'].at[2], s['ra'].at[2], s['rb'].at[2], s['r'].at[2], s['ss'].at[2], s['sr'].at[2])
    rs_d.start()

    ag_o = Gather(ring, s['bo'], s['oss'], s['ors'], s['ods'], s['oes'])
    s['bo'][core, chip] = pack(mine(s['e24'][...]) + rs_y.finish())
    ag_o.start()
    rs_d.middle()
    ag_o.first()

    def own(v):
        return jnp.where(core == 0, v[:, :f_loc], v[:, f_loc:])

    hid_own = own(s['hid'][...].astype(F32)).astype(BF)
    for i in range(2):
        acc = jnp.zeros((f_loc, half), F32)
        for j in (2, 1, 0):
            acc = acc + dot(hid_own, s['sp'][3 * i + j], 0, 0)
        if i == 0:
            s['dw2'][:, :half] = acc
        else:
            s['dw2'][:, half:] = acc[:, :rest]
    o_w2 = local(s['dw2'], dw2_ref, 6)
    o_w2.start()

    rs_d.short()
    ag_o.middle()
    du_own = parts(own(du))
    for i in range(2):
        acc = jnp.zeros((f_loc, half), F32)
        for p in du_own[::-1]:
            acc = acc + dot(p, s['n'][i], 0, 0)
        if i == 0:
            s['dw1'][:, :half] = acc
        else:
            s['dw1'][:, half:] = acc[:, :rest]
    o_w1 = local(s['dw1'], dw1_ref, 7)
    o_w1.start()

    s['dnx'][core] = rs_d.finish()
    r_dn = pair(s['dnx'].at[core], s['dnx'].at[core], 5)
    r_dn.start()
    ag_o.last()
    pair(s['dnx'].at[1 - core], s['dnx'].at[1 - core], 5).wait_recv()
    inv = inv_rms(s['e24'][...])
    xr = s['e24'][...] * inv
    gd = gain * jnp.concatenate([s['dnx'][0], s['dnx'][1]], axis=1)
    dx = inv * (gd - xr * (jnp.sum(xr * gd, axis=-1, keepdims=True) / width))
    dx = dx + jnp.concatenate([s['bs'][0, chip], s['bs'][1, chip]], axis=1)
    s['de'][...] = jnp.where(core == 0, dx[:rows_e], dx[rows_e:])[:, :width]
    o_de = local(s['de'], de_ref, 8)
    o_de.start()

    ag_o.finish()
    unpack(s['bo'], s['o'])
    mask = hot(s['ids'][core])
    s['out'][:half] = dot(s['o'][0], mask, 0, 0).astype(BF)
    s['out'][half:] = dot(s['o'][1], mask, 0, 0)[:rest].astype(BF)
    o_out = local(s['out'], out_ref, 9)
    o_out.start()

    for c in (r_e, r_i, r_w1, r_w2, r_dn):
        c.wait_send()
    for i in range(2):
        @pl.when(core == i)
        def _():
            d_give[i].wait_send()
    for x in (ag_n, rs_s, ag_s, rs_y, rs_d, ag_o):
        x.drain()
    for c in (o_w2, o_w1, o_de, o_out):
        c.wait()


def solution(mesh):
    tok_spec = P(('data', 'tensor'))
    row_spec = P(('data', 'tensor'), None)
    n_tensor = mesh.shape['tensor']
    chips = n_tensor // CORES
    side = math.isqrt(chips)
    assert side == 4 and side * side == chips

    def local_step(token_ids, emb_shard, norm_gain, w_up, w_down, grad_out):
        rows_e, width = emb_shard.shape
        tokens = token_ids.shape[0]
        f_loc = w_up.shape[1]
        f_chip = CORES * f_loc
        half = -(-width // 256) * 128
        rb = CORES * rows_e
        vocab = chips * rb
        vm = pltpu.VMEM
        dma = lambda *shape: pltpu.SemaphoreType.DMA(shape)
        scratch = dict(
            es=vm((2, rows_e, width), BF), gsrc=vm((1, width), BF), ids=vm((2, 1, tokens), jnp.int32),
            w1s=vm((2, f_loc, width), BF), w2s=vm((2, f_loc, width), BF), dt=vm((2, half, tokens), BF),
            e24=vm((rb, 2 * half), F32), w1p=vm((2, f_chip, half), BF), w2p=vm((2, f_chip, half), BF),
            bn=vm((2, chips, 2 * rb, half // 2), BF), bo=vm((2, chips, 2 * rb, half // 2), BF),
            bs=vm((2, chips, rb, half), F32), sp=vm((6, vocab, half), BF),
            n=vm((2, vocab, half), BF), o=vm((2, vocab, half), BF),
            gs=vm((chips, rb, half), F32), gy=vm((chips, rb, half), F32), gd=vm((chips, rb, half), F32),
            lay=vm((3, 4, rb, half), F32), ra=vm((3, 2, 4, rb, half), F32), rb=vm((3, 3, rb, half), F32),
            r=vm((3, 4, rb, half), F32),
            hid=vm((vocab, f_chip), BF), slope=vm((vocab, f_chip), F32),
            dnx=vm((2, rb, half), F32), de=vm((rows_e, width), F32),
            dw1=vm((f_loc, width), F32), dw2=vm((f_loc, width), F32), out=vm((width, tokens), BF),
            lsem=dma(10), psem=dma(6), qsem=dma(6),
            ss=dma(3, 15), sr=dma(3, 15),
        )
        for name in 'nso':
            scratch.update({name + 'ss': dma(15), name + 'rs': dma(15), name + 'ds': dma(chips), name + 'es': dma(chips)})
        names = list(scratch)

        def body(*refs):
            kernel(side, *refs[:10], dict(zip(names, refs[10:])))

        hbm = pl.BlockSpec(memory_space=pl.ANY)
        out_t, d_emb, dw1_t, d_w2 = pl.pallas_call(
            body,
            out_shape=(
                jax.ShapeDtypeStruct((width, tokens), BF),
                jax.ShapeDtypeStruct((rows_e, width), F32),
                jax.ShapeDtypeStruct((f_loc, width), F32),
                jax.ShapeDtypeStruct((f_loc, width), F32),
            ),
            in_specs=[hbm] * 6,
            out_specs=(hbm,) * 4,
            scratch_shapes=list(scratch.values()),
            compiler_params=pltpu.CompilerParams(
                collective_id=0, has_side_effects=True, vmem_limit_bytes=60 * 1024 * 1024),
            name='step',
        )(token_ids.reshape(1, tokens), emb_shard, norm_gain.reshape(1, width), w_up.T, w_down, grad_out.T)
        return out_t.T, d_emb, dw1_t.T, d_w2

    return jax.shard_map(
        local_step,
        mesh=mesh,
        in_specs=(tok_spec, P('tensor', None), P(None), P(None, 'tensor'), P('tensor', None), row_spec),
        out_specs=(row_spec, row_spec, P('data', 'tensor'), row_spec),
        check_vma=False,
    )
```

```python
import functools
import math

import jax
import jax.numpy as jnp
from jax import lax
from jax.experimental import pallas as pl
from jax.experimental.pallas import tpu as pltpu
from jax.sharding import PartitionSpec as P

EPS = 1e-6
BF = jnp.bfloat16
F32 = jnp.float32
CORES = 2
MESH = pl.DeviceIdType.MESH


def gelu_tanh(values):
    return jax.nn.gelu(values, approximate=True)


def parts(v):
    hi = v.astype(BF)
    r = v - hi.astype(F32)
    mid = r.astype(BF)
    lo = (r - mid.astype(F32)).astype(BF)
    return hi, mid, lo


def dot(a, b, ca, cb):
    return lax.dot_general(a, b, (((ca,), (cb,)), ((), ())), preferred_element_type=F32)


def pack(v):
    half = v.shape[1] // 2
    return jnp.concatenate([v[:, :half], v[:, half:]], axis=0).astype(BF)


def hot(ids_row, vocab):
    row = lax.broadcasted_iota(jnp.int32, (vocab, ids_row.shape[1]), 0)
    return jnp.where(row == ids_row, 1.0, 0.0).astype(BF)


class Ring:
    def __init__(self, side):
        me = lax.axis_index('tensor')
        self.side = side
        self.core = core = lax.rem(me, CORES)
        self.chip = chip = me // CORES
        x, y = lax.rem(chip, side), chip // side
        self.a = x * (1 - core) + y * core
        self.b = y * (1 - core) + x * core
        self.partner = {'tensor': me + 1 - 2 * core}

    def at(self, da, db):
        a = lax.rem(self.a + da, self.side)
        b = lax.rem(self.b + db, self.side)
        return a * (1 + (self.side - 1) * self.core) + b * (self.side - (self.side - 1) * self.core)

    def dev(self, da, db):
        return {'tensor': self.at(da, db) * CORES + self.core}


PLUS, MINUS = (2, 1), (3, 0)


class Scatter:
    def __init__(self, ring, g, relay, ra, rb, r, ssem, rsem):
        self.ring, self.g, self.relay, self.ra, self.rb, self.r = ring, g, relay, ra, rb, r
        self.ssem, self.rsem = ssem, rsem
        self.sent = []

    def copy(self, src, dst, i, dev):
        return pltpu.make_async_remote_copy(
            src_ref=src, dst_ref=dst, send_sem=self.ssem, recv_sem=self.rsem.at[i],
            device_id=dev, device_id_type=MESH)

    def c_relay(self, k):
        da = 1 if k in PLUS else 3
        return self.copy(self.g.at[self.ring.at(2, k)], self.relay.at[k], k, self.ring.dev(da, 0))

    def c_ring(self, k, plus):
        da = 1 if plus else 3
        j = 0 if plus else 1
        return self.copy(self.g.at[self.ring.at(da, k)], self.ra.at[j, k], 4 + 4 * j + k, self.ring.dev(da, 0))

    def c_b(self, k):
        return self.copy(self.r.at[k], self.rb.at[k - 1], 11 + k, self.ring.dev(0, k))

    def go(self, c):
        c.start()
        self.sent.append(c)

    def start_relay(self):
        for kp, km in zip(PLUS, MINUS):
            self.go(self.c_relay(kp))
            self.go(self.c_relay(km))

    def start_own(self):
        for kp, km in zip(MINUS, PLUS):
            self.go(self.c_ring(kp, True))
            self.go(self.c_ring(km, False))

    def middle(self):
        for kp, km in zip(PLUS, MINUS):
            for k, plus in ((kp, True), (km, False)):
                self.c_relay(k).wait_recv()
                blk = self.ring.at(1 if plus else 3, k)
                self.g[blk] = self.g[blk] + self.relay[k]
                self.go(self.c_ring(k, plus))

    def short(self):
        for k in (2, 3, 1, 0):
            self.c_ring(k, True).wait_recv()
            self.c_ring(k, False).wait_recv()
            self.r[k] = self.g[self.ring.at(0, k)] + self.ra[0, k] + self.ra[1, k]
            if k:
                self.go(self.c_b(k))

    def finish(self):
        acc = self.r[0]
        for k in (1, 3, 2):
            self.c_b(k).wait_recv()
            acc = acc + self.rb[k - 1]
        return acc

    def drain(self):
        whole = self.g.at[pl.ds(0, len(self.sent))]
        pltpu.make_async_copy(whole, whole, self.ssem).wait()


FWD_P, FWD_M = (0, 2), (3, 1)


class Gather:
    def __init__(self, ring, buf, ssem, rsem, dsem, esem):
        self.ring, self.buf = ring, buf
        self.ssem, self.rsem, self.dsem, self.esem = ssem, rsem, dsem, esem
        self.sent = []

    def copy(self, blk, i, dev):
        ref = self.buf.at[self.ring.core, blk]
        return pltpu.make_async_remote_copy(
            src_ref=ref, dst_ref=ref, send_sem=self.ssem, recv_sem=self.rsem.at[i],
            device_id=dev, device_id_type=MESH)

    def back(self, k):
        return (self.ring.side - k) % self.ring.side

    def go(self, c):
        c.start()
        self.sent.append(c)

    def over(self, blk, stage):
        ref = self.buf.at[self.ring.core, blk]
        pltpu.make_async_remote_copy(
            src_ref=ref, dst_ref=ref, send_sem=self.esem, recv_sem=self.dsem.at[stage],
            device_id=self.ring.partner, device_id_type=MESH).start()

    def both(self, k):
        blk = self.ring.at(0, self.back(k))
        self.go(self.copy(blk, k, self.ring.dev(1, 0)))
        self.go(self.copy(blk, 4 + k, self.ring.dev(3, 0)))

    def start(self):
        blk = self.ring.at(0, 0)
        for k in (2, 1, 3):
            self.go(self.copy(blk, 11 + k, self.ring.dev(0, k)))
        self.both(0)
        self.over(blk, 0)

    def first(self):
        for k in (1, 3, 2):
            blk = self.ring.at(0, self.back(k))
            self.copy(blk, 11 + k, self.ring.dev(0, k)).wait_recv()
            self.both(k)
            self.over(blk, 0)

    def middle(self, ks=(0, 1, 3, 2)):
        for k in ks:
            blk = self.ring.at(3, self.back(k))
            self.copy(blk, k, self.ring.dev(1, 0)).wait_recv()
            if k in FWD_P:
                self.go(self.copy(blk, 8 + k, self.ring.dev(1, 0)))
            self.over(blk, 1)
            blk = self.ring.at(1, self.back(k))
            self.copy(blk, 4 + k, self.ring.dev(3, 0)).wait_recv()
            if k in FWD_M:
                self.go(self.copy(blk, 8 + k, self.ring.dev(3, 0)))
            self.over(blk, 1)

    def last(self):
        for k in (0, 3, 1, 2):
            blk = self.ring.at(2, self.back(k))
            self.copy(blk, 8 + k, self.ring.dev(1, 0)).wait_recv()
            self.over(blk, 2)

    def passed(self, stage):
        ref = self.buf.at[1 - self.ring.core, pl.ds(0, (4, 8, 4)[stage])]
        pltpu.make_async_copy(ref, ref, self.dsem.at[stage]).wait()

    def finish(self):
        for stage in range(3):
            self.passed(stage)

    def drain(self):
        ref = self.buf.at[self.ring.core]
        pltpu.make_async_copy(ref, ref, self.esem).wait()
        ref = self.buf.at[0, pl.ds(0, len(self.sent))]
        pltpu.make_async_copy(ref, ref, self.ssem).wait()


def kernel(side, ids_in, e_in, g_in, w1_in, w2_in, d_in, o_ref, de_ref, dw1_ref, dw2_ref, s):
    ring = Ring(side)
    core, chip, partner = ring.core, ring.chip, ring.partner
    chips = side * side
    rows_e, width = e_in.shape
    f_loc = w1_in.shape[0]
    f_chip = CORES * f_loc
    half = s['w1p'].shape[2]
    rest = width - half
    rb = s['gs'].shape[1]
    vocab = chips * rb

    def local(src, dst, i):
        return pltpu.make_async_copy(src, dst, s['lsem'].at[i])

    def pair(src, dst, i):
        return pltpu.make_async_remote_copy(
            src_ref=src, dst_ref=dst, send_sem=s['psem'].at[i], recv_sem=s['qsem'].at[i],
            device_id=partner, device_id_type=MESH)

    c_e = local(e_in, s['es'].at[core], 0)
    c_g = local(g_in, s['gsrc'], 1)
    c_i = local(ids_in, s['ids'].at[core], 2)
    c_w1 = local(w1_in, s['w1s'].at[core], 3)
    c_w2 = local(w2_in, s['w2s'].at[core], 4)
    d_own = (local(d_in.at[:half], s['dt'].at[0], 5),
             local(d_in.at[half:], s['dt'].at[0, :rest], 5))
    r_e = pair(e_in, s['es'].at[core], 0)
    r_i = pair(ids_in, s['ids'].at[core], 1)
    r_w1 = pair(w1_in, s['w1s'].at[core], 2)
    r_w2 = pair(w2_in, s['w2s'].at[core], 3)
    d_give = (pair(d_in.at[half:], s['dt'].at[1, :rest], 4),
              pair(d_in.at[:half], s['dt'].at[1], 4))

    for c in (c_e, c_g, c_i):
        c.start()

    @pl.when(core == 1)
    def _():
        for j in range(2):
            s['dt'][j, rest:, :] = jnp.zeros((half - rest, s['dt'].shape[2]), BF)

    barrier = pltpu.get_barrier_semaphore()
    peers = [partner, ring.dev(1, 0), ring.dev(3, 0)] + [ring.dev(0, k) for k in (1, 2, 3)]
    for p in peers:
        pl.semaphore_signal(barrier, inc=1, device_id=p, device_id_type=MESH)
    for i in range(2):
        @pl.when(core == i)
        def _():
            d_own[i].start()
    c_w1.start()
    c_w2.start()
    pl.semaphore_wait(barrier, len(peers))

    r_e.start()
    r_i.start()
    for i in range(2):
        @pl.when(core == i)
        def _():
            d_give[i].start()
    r_w1.start()
    r_w2.start()

    def wide(v):
        return jnp.concatenate([v, jnp.zeros((v.shape[0], 2 * half - width), F32)], axis=1)

    c_e.wait()
    c_g.wait()
    r_e.wait_recv()
    gain = wide(s['gsrc'][...].astype(F32).reshape(1, width))
    for i in range(2):
        s['e24'][i * rows_e:(i + 1) * rows_e, :] = wide(s['es'][i].astype(F32))

    def inv_rms(x):
        return lax.rsqrt(jnp.sum(x * x, axis=-1, keepdims=True) / width + EPS)

    def mine(v):
        return jnp.where(core == 0, v[:, :half], v[:, half:])

    x24 = s['e24'][...]
    ag_n = Gather(ring, s['bn'], s['gsem'].at[3], s['gr'].at[0], s['gd3'].at[0], s['gsem'].at[6])
    s['bn'][core, chip] = pack(mine(x24 * inv_rms(x24) * gain))
    ag_n.start()

    c_i.wait()
    for i in range(2):
        @pl.when(core == i)
        def _():
            d_own[i].wait()
    tot = dot(hot(s['ids'][core], vocab), s['dt'][0], 1, 1)
    r_i.wait_recv()
    for i in range(2):
        @pl.when(core == i)
        def _():
            d_give[1 - i].wait_recv()

    tot = tot + dot(hot(s['ids'][1 - core], vocab), s['dt'][1], 1, 1)
    s['gs'][...] = tot.reshape(chips, rb, half)
    rs_s = Scatter(ring, s['gs'], s['lay'].at[0], s['ra'].at[0], s['rb'].at[0], s['r'].at[0], s['gsem'].at[0], s['sr'].at[0])
    rs_s.start_relay()
    rs_s.start_own()

    ag_n.first()

    c_w1.wait()
    c_w2.wait()
    r_w1.wait_recv()
    r_w2.wait_recv()
    for w_src, w_dst in (('w1s', 'w1p'), ('w2s', 'w2p')):
        for i in range(2):
            rows = slice(i * f_loc, (i + 1) * f_loc)
            s[w_dst][0, rows, :] = s[w_src][i, :, :half]
            s[w_dst][1, rows, :] = jnp.concatenate(
                [s[w_src][i, :, half:], jnp.zeros((f_loc, half - rest), BF)], axis=1)

    rs_s.middle()
    ag_n.middle()
    rs_s.short()
    ag_n.last()
    ag_n.finish()

    def unpack(buf, dst):
        q = half // 2
        for h in range(2):
            v = buf[h].astype(F32)
            dst[h, :, :q] = v[:, :rb].reshape(vocab, q).astype(BF)
            dst[h, :, q:] = v[:, rb:].reshape(vocab, q).astype(BF)

    unpack(s['bn'], s['n'])
    pre = (dot(s['n'][0], s['w1p'][0], 1, 1) + dot(s['n'][1], s['w1p'][1], 1, 1)).astype(BF)
    pre_f = pre.astype(F32)
    act, gelu_back = jax.vjp(gelu_tanh, pre_f)
    hid = act.astype(BF)
    s['hid'][...] = hid
    s['slope'][...] = gelu_back(jnp.ones_like(pre_f))[0].reshape(chips, rb, f_chip)
    s['dh'][...] = jnp.zeros((chips, rb, f_chip), F32)
    s['gy'][...] = dot(hid, s['w2p'][core], 1, 0).reshape(chips, rb, half)

    rs_y = Scatter(ring, s['gy'], s['lay'].at[1], s['ra'].at[1], s['rb'].at[1], s['r'].at[1], s['gsem'].at[1], s['sr'].at[1])
    ag_s = Gather(ring, s['bs'], s['gsem'].at[4], s['gr'].at[1], s['gd3'].at[1], s['gsem'].at[7])
    s['bs'][core, chip] = rs_s.finish()
    ag_s.start()
    rs_y = Scatter(ring, s['gy'], s['lay'].at[1], s['ra'].at[1], s['rb'].at[1], s['r'].at[1], s['gsem'].at[1], s['sr'].at[1])
    rs_y.start_relay()
    rs_y.start_own()
    ag_s.first()

    def tall(v):
        return jnp.concatenate(parts(v), axis=0)

    def short(v):
        n = v.shape[0] // 3
        return v[2 * n:] + v[n:2 * n] + v[:n]

    def dh_add(h, blks):
        v = jnp.concatenate([s['bs'][h, blk] for blk in blks], axis=0)
        d = short(dot(tall(v), s['w2p'][h], 1, 1))
        for i, blk in enumerate(blks):
            s['dh'][blk] = s['dh'][blk] + d[i * rb:(i + 1) * rb]

    def line(da):
        return [ring.at(da, k) for k in range(side)]

    def cross(db):
        return [ring.at(k, db) for k in range(side)]

    def dn_rows(da):
        blks = line(da)
        du = [s['dh'][blk] * s['slope'][blk] for blk in blks]
        for blk, v in zip(blks, du):
            s['dh'][blk] = v
        d = short(dot(tall(jnp.concatenate(du, axis=0)), s['w1p'][core], 1, 0))
        for i, blk in enumerate(blks):
            s['gd'][blk] = d[i * rb:(i + 1) * rb]

    ag_s.middle((0,))
    dh_add(core, line(0))
    rs_y.middle()
    ag_s.middle((1, 3, 2))
    dh_add(core, line(1) + line(3))
    ag_s.passed(0)
    dh_add(1 - core, cross(0))
    rs_y.short()
    ag_s.passed(1)
    dh_add(1 - core, cross(1) + cross(3))
    ag_s.last()
    dh_add(core, line(2))
    ag_s.passed(2)
    dh_add(1 - core, cross(2))
    rs_d = Scatter(ring, s['gd'], s['lay'].at[2], s['ra'].at[2], s['rb'].at[2], s['r'].at[2], s['gsem'].at[2], s['sr'].at[2])
    dn_rows(2)
    rs_d.start_relay()
    dn_rows(1)
    dn_rows(3)
    rs_d.start_own()
    dn_rows(0)
    ag_o = Gather(ring, s['bo'], s['gsem'].at[5], s['gr'].at[2], s['gd3'].at[2], s['gsem'].at[8])
    s['bo'][core, chip] = pack(mine(s['e24'][...]) + rs_y.finish())
    ag_o.start()
    for i in range(2):
        for j, p in enumerate(parts(s['bs'][i].reshape(vocab, half))):
            s['sp'][3 * i + j] = p

    def own(v):
        return jnp.where(core == 0, v[:, :f_loc], v[:, f_loc:])

    hid_own = own(s['hid'][...].astype(F32)).astype(BF)
    for i in range(2):
        acc = jnp.zeros((f_loc, half), F32)
        for j in (2, 1, 0):
            acc = acc + dot(hid_own, s['sp'][3 * i + j], 0, 0)
        if i == 0:
            dw2_ref[:, :half] = acc
        else:
            dw2_ref[:, half:] = acc[:, :rest]

    rs_d.middle()
    ag_o.first()

    du_own = parts(own(s['dh'][...].reshape(vocab, f_chip)))
    for i in range(2):
        acc = jnp.zeros((f_loc, half), F32)
        for p in du_own[::-1]:
            acc = acc + dot(p, s['n'][i], 0, 0)
        if i == 0:
            dw1_ref[:, :half] = acc
        else:
            dw1_ref[:, half:] = acc[:, :rest]

    rs_d.short()
    ag_o.middle()
    s['dnx'][core] = rs_d.finish()
    r_dn = pair(s['dnx'].at[core], s['dnx'].at[core], 5)
    r_dn.start()
    ag_o.last()
    pair(s['dnx'].at[1 - core], s['dnx'].at[1 - core], 5).wait_recv()
    inv = inv_rms(s['e24'][...])
    xr = s['e24'][...] * inv
    gd = gain * jnp.concatenate([s['dnx'][0], s['dnx'][1]], axis=1)
    dx = inv * (gd - xr * (jnp.sum(xr * gd, axis=-1, keepdims=True) / width))
    dx = dx + jnp.concatenate([s['bs'][0, chip], s['bs'][1, chip]], axis=1)
    de_ref[...] = jnp.where(core == 0, dx[:rows_e], dx[rows_e:])[:, :width]

    ag_o.finish()
    unpack(s['bo'], o_ref)

    for c in (r_e, r_i, r_w1, r_w2, r_dn):
        c.wait_send()
    for i in range(2):
        @pl.when(core == i)
        def _():
            d_give[i].wait_send()
    for x in (ag_n, rs_s, ag_s, rs_y, rs_d, ag_o):
        x.drain()


def rows_out(ids, o, de, dw1, dw2, out_ref, de_ref, dw1_ref, dw2_ref, buf, sem):
    copies = [pltpu.make_async_copy(src, dst, sem.at[i]) for i, (src, dst) in enumerate(
        ((dw1, dw1_ref), (dw2, dw2_ref), (de, de_ref), (buf, out_ref)))]
    for c in copies[:3]:
        c.start()
    _, vocab, half = o.shape
    mask = hot(ids[...], vocab)
    buf[:half] = dot(o[0], mask, 0, 0).astype(BF)
    buf[half:] = dot(o[1], mask, 0, 0)[:buf.shape[0] - half].astype(BF)
    copies[3].start()
    for c in copies:
        c.wait()


def solution(mesh):
    tok_spec = P(('data', 'tensor'))
    row_spec = P(('data', 'tensor'), None)
    n_tensor = mesh.shape['tensor']
    chips = n_tensor // CORES
    side = math.isqrt(chips)
    assert side == 4 and side * side == chips

    def local_step(token_ids, emb_shard, norm_gain, w_up, w_down, grad_out):
        rows_e, width = emb_shard.shape
        tokens = token_ids.shape[0]
        f_loc = w_up.shape[1]
        f_chip = CORES * f_loc
        half = -(-width // 256) * 128
        rb = CORES * rows_e
        vocab = chips * rb
        vm = pltpu.VMEM
        dma = lambda *shape: pltpu.SemaphoreType.DMA(shape)
        scratch = dict(
            es=vm((2, rows_e, width), BF), gsrc=vm((width,), BF), ids=vm((2, 1, tokens), jnp.int32),
            w1s=vm((2, f_loc, width), BF), w2s=vm((2, f_loc, width), BF), dt=vm((2, half, tokens), BF),
            e24=vm((rb, 2 * half), F32), w1p=vm((2, f_chip, half), BF), w2p=vm((2, f_chip, half), BF),
            bn=vm((2, chips, 2 * rb, half // 2), BF), bo=vm((2, chips, 2 * rb, half // 2), BF),
            bs=vm((2, chips, rb, half), F32), sp=vm((6, vocab, half), BF),
            n=vm((2, vocab, half), BF),
            gs=vm((chips, rb, half), F32), gy=vm((chips, rb, half), F32), gd=vm((chips, rb, half), F32),
            lay=vm((3, 4, rb, half), F32), ra=vm((3, 2, 4, rb, half), F32), rb=vm((3, 3, rb, half), F32),
            r=vm((3, 4, rb, half), F32),
            hid=vm((vocab, f_chip), BF), slope=vm((chips, rb, f_chip), F32), dh=vm((chips, rb, f_chip), F32),
            dnx=vm((2, rb, half), F32),
            lsem=dma(6), psem=dma(6), qsem=dma(6),
            gsem=dma(9), gd3=dma(3, 3), sr=dma(3, 15), gr=dma(3, 15),
        )
        names = list(scratch)

        def body(*refs):
            kernel(side, *refs[:10], dict(zip(names, refs[10:])))

        hbm = pl.BlockSpec(memory_space=pltpu.HBM)
        on_chip = pl.BlockSpec(memory_space=pltpu.VMEM)
        shapes = (
            jax.ShapeDtypeStruct((rows_e, width), F32),
            jax.ShapeDtypeStruct((f_loc, width), F32),
            jax.ShapeDtypeStruct((f_loc, width), F32),
        )
        ids_row = token_ids.reshape(1, tokens)
        done = pl.pallas_call(
            body,
            out_shape=(jax.ShapeDtypeStruct((2, vocab, half), BF),) + shapes,
            in_specs=[hbm] * 6,
            out_specs=(on_chip,) * 4,
            scratch_shapes=list(scratch.values()),
            compiler_params=pltpu.CompilerParams(
                collective_id=0, has_side_effects=True, vmem_limit_bytes=36 * 1024 * 1024),
            name='step',
        )(*(pltpu.with_memory_space_constraint(v, pltpu.HBM) for v in (
            ids_row, emb_shard, norm_gain, w_up.T, w_down, grad_out.T)))
        out_t, d_emb, dw1_t, d_w2 = pl.pallas_call(
            rows_out,
            out_shape=(jax.ShapeDtypeStruct((width, tokens), BF),) + shapes,
            in_specs=[on_chip] * 5,
            out_specs=(hbm,) * 4,
            scratch_shapes=[vm((width, tokens), BF), dma(4)],
            compiler_params=pltpu.CompilerParams(vmem_limit_bytes=16 * 1024 * 1024),
            name='rows_out',
        )(ids_row, *done)
        return out_t.T, d_emb, dw1_t.T, d_w2

    return jax.shard_map(
        local_step,
        mesh=mesh,
        in_specs=(tok_spec, P('tensor', None), P(None), P(None, 'tensor'), P('tensor', None), row_spec),
        out_specs=(row_spec, row_spec, P('data', 'tensor'), row_spec),
        check_vma=False,
    )
```

```python
import functools
import math

import jax
import jax.numpy as jnp
from jax import lax
from jax.experimental import pallas as pl
from jax.experimental.pallas import tpu as pltpu
from jax.sharding import PartitionSpec as P

EPS = 1e-6
BF = jnp.bfloat16
F32 = jnp.float32
CORES = 2
MESH = pl.DeviceIdType.MESH


def gelu_tanh(values):
    return jax.nn.gelu(values, approximate=True)


def parts(v):
    hi = v.astype(BF)
    r = v - hi.astype(F32)
    mid = r.astype(BF)
    lo = (r - mid.astype(F32)).astype(BF)
    return hi, mid, lo


def dot(a, b, ca, cb):
    return lax.dot_general(a, b, (((ca,), (cb,)), ((), ())), preferred_element_type=F32)


def pack(v):
    half = v.shape[1] // 2
    return jnp.concatenate([v[:, :half], v[:, half:]], axis=0).astype(BF)


def hot(ids_row, vocab):
    row = lax.broadcasted_iota(jnp.int32, (vocab, ids_row.shape[1]), 0)
    return jnp.where(row == ids_row, 1.0, 0.0).astype(BF)


class Ring:
    def __init__(self, side):
        me = lax.axis_index('tensor')
        self.side = side
        self.core = core = lax.rem(me, CORES)
        self.chip = chip = me // CORES
        x, y = lax.rem(chip, side), chip // side
        self.a = x * (1 - core) + y * core
        self.b = y * (1 - core) + x * core
        self.partner = {'tensor': me + 1 - 2 * core}

    def at(self, da, db):
        a = lax.rem(self.a + da, self.side)
        b = lax.rem(self.b + db, self.side)
        return a * (1 + (self.side - 1) * self.core) + b * (self.side - (self.side - 1) * self.core)

    def dev(self, da, db):
        return {'tensor': self.at(da, db) * CORES + self.core}


PLUS, MINUS = (2, 1), (3, 0)


class Scatter:
    def __init__(self, ring, g, relay, ra, rb, r, ssem, rsem):
        self.ring, self.g, self.relay, self.ra, self.rb, self.r = ring, g, relay, ra, rb, r
        self.ssem, self.rsem = ssem, rsem
        self.sent = []

    def copy(self, src, dst, i, dev):
        return pltpu.make_async_remote_copy(
            src_ref=src, dst_ref=dst, send_sem=self.ssem, recv_sem=self.rsem.at[i],
            device_id=dev, device_id_type=MESH)

    def c_relay(self, k):
        da = 1 if k in PLUS else 3
        return self.copy(self.g.at[self.ring.at(2, k)], self.relay.at[k], k, self.ring.dev(da, 0))

    def c_ring(self, k, plus):
        da = 1 if plus else 3
        j = 0 if plus else 1
        return self.copy(self.g.at[self.ring.at(da, k)], self.ra.at[j, k], 4 + k, self.ring.dev(da, 0))

    def c_b(self, k):
        return self.copy(self.r.at[k], self.rb.at[k - 1], 8, self.ring.dev(0, k))

    def go(self, c):
        c.start()
        self.sent.append(c)

    def relays(self, j):
        for kp, km in ((PLUS[j], MINUS[j]),):
            self.go(self.c_relay(kp))
            self.go(self.c_relay(km))

    def owns(self, j):
        for kp, km in ((MINUS[j], PLUS[j]),):
            self.go(self.c_ring(kp, True))
            self.go(self.c_ring(km, False))

    def middle(self, j):
        for kp, km in ((PLUS[j], MINUS[j]),):
            for k, plus in ((kp, True), (km, False)):
                self.c_relay(k).wait_recv()
                blk = self.ring.at(1 if plus else 3, k)
                self.g[blk] = self.g[blk] + self.relay[k]
                self.go(self.c_ring(k, plus))

    def short(self, *ks):
        for k in ks:
            self.arrived(2, 4 + k)
            self.r[k] = self.g[self.ring.at(0, k)] + self.ra[0, k] + self.ra[1, k]
            if k:
                self.go(self.c_b(k))

    def finish(self):
        self.arrived(3, 8)
        return self.r[0] + self.rb[0] + self.rb[2] + self.rb[1]

    def arrived(self, blocks, i):
        ref = self.g.at[pl.ds(0, blocks)]
        pltpu.make_async_copy(ref, ref, self.rsem.at[i]).wait()

    def drain(self):
        whole = self.g.at[pl.ds(0, len(self.sent))]
        pltpu.make_async_copy(whole, whole, self.ssem).wait()


FWD_P, FWD_M = (0, 2), (3, 1)


class Gather:
    def __init__(self, ring, buf, ssem, rsem, dsem, esem, direct=False):
        self.ring, self.buf, self.direct = ring, buf, direct
        self.ssem, self.rsem, self.dsem, self.esem = ssem, rsem, dsem, esem
        self.sent = []

    def copy(self, blk, i, dev):
        ref = self.buf.at[self.ring.core, blk]
        return pltpu.make_async_remote_copy(
            src_ref=ref, dst_ref=ref, send_sem=self.ssem, recv_sem=self.rsem.at[i],
            device_id=dev, device_id_type=MESH)

    def back(self, k):
        return (self.ring.side - k) % self.ring.side

    def go(self, c):
        c.start()
        self.sent.append(c)

    def over(self, blk, stage):
        ref = self.buf.at[self.ring.core, blk]
        pltpu.make_async_remote_copy(
            src_ref=ref, dst_ref=ref, send_sem=self.esem, recv_sem=self.dsem.at[stage],
            device_id=self.ring.partner, device_id_type=MESH).start()

    def both(self, k):
        blk = self.ring.at(0, self.back(k))
        self.go(self.copy(blk, k, self.ring.dev(1, 0)))
        self.go(self.copy(blk, 4 + k, self.ring.dev(3, 0)))
        if self.direct:
            self.go(self.copy(blk, 8 + k, self.ring.dev(2, 0)))

    def start(self):
        blk = self.ring.at(0, 0)
        for k in (2, 1, 3):
            self.go(self.copy(blk, 11 + k, self.ring.dev(0, k)))
        self.both(0)
        self.over(blk, 0)

    def first(self, *ks):
        for k in ks:
            blk = self.ring.at(0, self.back(k))
            self.copy(blk, 11 + k, self.ring.dev(0, k)).wait_recv()
            self.both(k)
            self.over(blk, 0)

    def middle(self, *ks):
        for k in ks:
            blk = self.ring.at(3, self.back(k))
            self.copy(blk, k, self.ring.dev(1, 0)).wait_recv()
            if k in FWD_P and not self.direct:
                self.go(self.copy(blk, 8 + k, self.ring.dev(1, 0)))
            self.over(blk, 1)
            blk = self.ring.at(1, self.back(k))
            self.copy(blk, 4 + k, self.ring.dev(3, 0)).wait_recv()
            if k in FWD_M and not self.direct:
                self.go(self.copy(blk, 8 + k, self.ring.dev(3, 0)))
            self.over(blk, 1)

    def last(self, *ks):
        for k in ks:
            blk = self.ring.at(2, self.back(k))
            self.copy(blk, 8 + k, self.ring.dev(1, 0)).wait_recv()
            self.over(blk, 2)

    def passed(self, stage):
        ref = self.buf.at[1 - self.ring.core, pl.ds(0, (4, 8, 4)[stage])]
        pltpu.make_async_copy(ref, ref, self.dsem.at[stage]).wait()

    def finish(self):
        for stage in range(3):
            self.passed(stage)

    def drain(self):
        ref = self.buf.at[self.ring.core]
        pltpu.make_async_copy(ref, ref, self.esem).wait()
        ref = self.buf.at[0, pl.ds(0, len(self.sent))]
        pltpu.make_async_copy(ref, ref, self.ssem).wait()


def kernel(side, ids_in, e_in, g_in, w1_in, w2_in, d_in, o_ref, de_ref, dw1_ref, dw2_ref, s):
    ring = Ring(side)
    core, chip, partner = ring.core, ring.chip, ring.partner
    chips = side * side
    rows_e, width = e_in.shape
    f_loc = w1_in.shape[0]
    f_chip = CORES * f_loc
    half = s['w1p'].shape[2]
    rest = width - half
    rb = s['gs'].shape[1]
    vocab = chips * rb

    def local(src, dst, i):
        return pltpu.make_async_copy(src, dst, s['lsem'].at[i])

    def pair(src, dst, i):
        return pltpu.make_async_remote_copy(
            src_ref=src, dst_ref=dst, send_sem=s['psem'].at[i], recv_sem=s['qsem'].at[i],
            device_id=partner, device_id_type=MESH)

    c_e = local(e_in, s['es'].at[core], 0)
    c_g = local(g_in, s['gsrc'], 1)
    c_i = local(ids_in, s['ids'].at[core], 2)
    c_w1 = local(w1_in, s['w1s'].at[core], 3)
    c_w2 = local(w2_in, s['w2s'].at[core], 4)
    d_own = (local(d_in.at[:half], s['dt'].at[0], 5),
             local(d_in.at[half:], s['dt'].at[0, :rest], 5))
    r_e = pair(s['es'].at[core], s['es'].at[core], 0)
    r_i = pair(s['ids'].at[core], s['ids'].at[core], 1)
    r_w1 = pair(w1_in, s['w1s'].at[core], 2)
    r_w2 = pair(w2_in, s['w2s'].at[core], 3)
    d_load = (local(d_in.at[half:], s['dg'].at[:rest], 6),
              local(d_in.at[:half], s['dg'], 6))
    d_give = (pair(s['dg'].at[:rest], s['dt'].at[1, :rest], 4),
              pair(s['dg'], s['dt'].at[1], 4))

    c_e.start()
    for i in range(2):
        @pl.when(core == i)
        def _():
            d_load[i].start()
    c_g.start()
    c_i.start()

    @pl.when(core == 1)
    def _():
        for j in range(2):
            s['dt'][j, rest:, :] = jnp.zeros((half - rest, s['dt'].shape[2]), BF)

    barrier = pltpu.get_barrier_semaphore()
    peers = [partner, ring.dev(1, 0), ring.dev(3, 0)] + [ring.dev(0, k) for k in (1, 2, 3)]
    for p in peers:
        pl.semaphore_signal(barrier, inc=1, device_id=p, device_id_type=MESH)
    for i in range(2):
        @pl.when(core == i)
        def _():
            d_own[i].start()
    c_w1.start()
    c_w2.start()
    pl.semaphore_wait(barrier, len(peers))

    c_e.wait()
    r_e.start()
    for i in range(2):
        @pl.when(core == i)
        def _():
            d_load[i].wait()
            d_give[i].start()
    c_i.wait()
    r_i.start()
    r_w1.start()
    r_w2.start()

    def wide(v):
        return jnp.concatenate([v, jnp.zeros((v.shape[0], 2 * half - width), F32)], axis=1)

    c_g.wait()
    r_e.wait_recv()
    gain = wide(s['gsrc'][...].astype(F32).reshape(1, width))
    for i in range(2):
        s['e24'][i * rows_e:(i + 1) * rows_e, :] = wide(s['es'][i].astype(F32))

    def inv_rms(x):
        return lax.rsqrt(jnp.sum(x * x, axis=-1, keepdims=True) / width + EPS)

    def mine(v):
        return jnp.where(core == 0, v[:, :half], v[:, half:])

    x24 = s['e24'][...]
    ag_n = Gather(ring, s['bn'], s['gsem'].at[3], s['gr'].at[0], s['gd3'].at[0], s['gsem'].at[6])
    s['bn'][core, chip] = pack(mine(x24 * inv_rms(x24) * gain))
    ag_n.start()

    for i in range(2):
        @pl.when(core == i)
        def _():
            d_own[i].wait()
    def s_rows(da, src):
        blks = [ring.at(da, k) for k in range(side)]
        row = jnp.concatenate([rb * blk + lax.broadcasted_iota(jnp.int32, (rb, s['dt'].shape[2]), 0) for blk in blks], axis=0)
        pick = jnp.where(row == s['ids'][core if src == 0 else 1 - core], 1.0, 0.0).astype(BF)
        d = dot(pick, s['dt'][src], 1, 1)
        for i, blk in enumerate(blks):
            v = d[i * rb:(i + 1) * rb]
            s['gs'][blk] = v if src == 0 else s['gs'][blk] + v

    for da in range(side):
        s_rows(da, 0)
    r_i.wait_recv()
    for i in range(2):
        @pl.when(core == i)
        def _():
            d_give[1 - i].wait_recv()

    s_rows(2, 1)
    rs_s = Scatter(ring, s['gs'], s['lay'].at[0], s['ra'].at[0], s['rb'].at[0], s['r'].at[0], s['gsem'].at[0], s['sr'].at[0])
    rs_s.relays(0)
    rs_s.relays(1)
    s_rows(1, 1)
    s_rows(3, 1)
    rs_s.owns(0)
    rs_s.owns(1)
    s_rows(0, 1)


    def tall(v):
        return jnp.concatenate(parts(v), axis=0)

    def short(v):
        n = v.shape[0] // 3
        return v[2 * n:] + v[n:2 * n] + v[:n]

    def dh_add(h, blks):
        v = jnp.concatenate([s['bs'][h, blk] for blk in blks], axis=0)
        d = short(dot(tall(v), s['w2p'][h], 1, 1))
        for i, blk in enumerate(blks):
            s['dh'][blk] = s['dh'][blk] + d[i * rb:(i + 1) * rb]

    def line(da):
        return [ring.at(da, k) for k in range(side)]

    def cross(db):
        return [ring.at(k, db) for k in range(side)]

    def dn_rows(da):
        blks = line(da)
        du = [s['dh'][blk] * s['slope'][blk] for blk in blks]
        for blk, v in zip(blks, du):
            s['dh'][blk] = v
        d = short(dot(tall(jnp.concatenate(du, axis=0)), s['w1p'][core], 1, 0))
        for i, blk in enumerate(blks):
            s['gd'][blk] = d[i * rb:(i + 1) * rb]

    def own(v):
        return jnp.where(core == 0, v[:, :f_loc], v[:, f_loc:])

    c_w1.wait()
    c_w2.wait()
    r_w1.wait_recv()
    r_w2.wait_recv()
    for w_src, w_dst in (('w1s', 'w1p'), ('w2s', 'w2p')):
        for i in range(2):
            rows = slice(i * f_loc, (i + 1) * f_loc)
            s[w_dst][0, rows, :] = s[w_src][i, :, :half]
            s[w_dst][1, rows, :] = jnp.concatenate(
                [s[w_src][i, :, half:], jnp.zeros((f_loc, half - rest), BF)], axis=1)

    ag_n.first(1)
    ag_n.first(3)
    ag_n.first(2)
    rs_s.middle(0)
    rs_s.middle(1)
    ag_n.middle(0)
    ag_n.middle(1)
    ag_n.middle(3)
    ag_n.middle(2)
    rs_s.short(2)
    rs_s.short(3)
    rs_s.short(1)
    rs_s.short(0)
    ag_n.last(0)
    ag_n.last(3)
    ag_n.last(1)
    ag_n.last(2)
    ag_n.finish()

    def unpack(buf, dst):
        q = half // 2
        for h in range(2):
            v = buf[h].astype(F32)
            dst[h, :, :q] = v[:, :rb].reshape(vocab, q).astype(BF)
            dst[h, :, q:] = v[:, rb:].reshape(vocab, q).astype(BF)

    unpack(s['bn'], s['n'])
    pre = (dot(s['n'][0], s['w1p'][0], 1, 1) + dot(s['n'][1], s['w1p'][1], 1, 1)).astype(BF)
    pre_f = pre.astype(F32)
    act, gelu_back = jax.vjp(gelu_tanh, pre_f)
    hid = act.astype(BF)
    s['hid'][...] = hid
    s['slope'][...] = gelu_back(jnp.ones_like(pre_f))[0].reshape(chips, rb, f_chip)
    s['dh'][...] = jnp.zeros((chips, rb, f_chip), F32)
    s['gy'][...] = dot(hid, s['w2p'][core], 1, 0).reshape(chips, rb, half)

    ag_s = Gather(ring, s['bs'], s['gsem'].at[4], s['gr'].at[1], s['gd3'].at[1], s['gsem'].at[7])
    s['bs'][core, chip] = rs_s.finish()
    ag_s.start()
    rs_y = Scatter(ring, s['gy'], s['lay'].at[1], s['ra'].at[1], s['rb'].at[1], s['r'].at[1], s['gsem'].at[1], s['sr'].at[1])
    rs_y.relays(0)
    rs_y.relays(1)
    rs_y.owns(0)
    rs_y.owns(1)
    ag_s.first(1)
    ag_s.first(3)
    ag_s.first(2)
    ag_s.middle(0)
    dh_add(core, line(0))
    rs_y.middle(0)
    rs_y.middle(1)
    ag_s.middle(1)
    ag_s.middle(3)
    ag_s.middle(2)
    dh_add(core, line(1) + line(3))
    ag_s.passed(0)
    dh_add(1 - core, cross(0))
    rs_y.short(2)
    rs_y.short(3)
    rs_y.short(1)
    rs_y.short(0)
    ag_s.passed(1)
    dh_add(1 - core, cross(1) + cross(3))
    ag_s.last(0)
    ag_s.last(3)
    ag_s.last(1)
    ag_s.last(2)
    dh_add(core, line(2))
    ag_s.passed(2)
    dh_add(1 - core, cross(2))
    rs_d = Scatter(ring, s['gd'], s['lay'].at[2], s['ra'].at[2], s['rb'].at[2], s['r'].at[2], s['gsem'].at[2], s['sr'].at[0])
    dn_rows(2)
    rs_d.relays(0)
    rs_d.relays(1)
    dn_rows(1)
    dn_rows(3)
    rs_d.owns(0)
    rs_d.owns(1)
    dn_rows(0)
    ag_o = Gather(ring, s['bo'], s['gsem'].at[5], s['gr'].at[0], s['gd3'].at[0], s['gsem'].at[8])
    s['bo'][core, chip] = pack(mine(s['e24'][...]) + rs_y.finish())
    ag_o.start()
    for i in range(2):
        for j, p in enumerate(parts(s['bs'][i].reshape(vocab, half))):
            s['sp'][3 * i + j] = p

    hid_own = own(s['hid'][...].astype(F32)).astype(BF)
    for i in range(2):
        acc = jnp.zeros((f_loc, half), F32)
        for j in (2, 1, 0):
            acc = acc + dot(hid_own, s['sp'][3 * i + j], 0, 0)
        if i == 0:
            dw2_ref[:, :half] = acc
        else:
            dw2_ref[:, half:] = acc[:, :rest]

    rs_d.middle(0)
    rs_d.middle(1)
    ag_o.first(1)
    ag_o.first(3)
    ag_o.first(2)
    rs_d.short(2)
    rs_d.short(3)
    rs_d.short(1)
    du_own = parts(own(s['dh'][...].reshape(vocab, f_chip)))
    for i in range(2):
        acc = jnp.zeros((f_loc, half), F32)
        for p in du_own[::-1]:
            acc = acc + dot(p, s['n'][i], 0, 0)
        if i == 0:
            dw1_ref[:, :half] = acc
        else:
            dw1_ref[:, half:] = acc[:, :rest]

    rs_d.short(0)
    ag_o.middle(0)
    ag_o.middle(1)
    ag_o.middle(3)
    ag_o.middle(2)
    s['dnx'][core] = rs_d.finish()
    r_dn = pair(s['dnx'].at[core], s['dnx'].at[core], 5)
    r_dn.start()
    ag_o.last(0)
    ag_o.last(3)
    ag_o.last(1)
    ag_o.last(2)
    pair(s['dnx'].at[1 - core], s['dnx'].at[1 - core], 5).wait_recv()
    inv = inv_rms(s['e24'][...])
    xr = s['e24'][...] * inv
    gd = gain * jnp.concatenate([s['dnx'][0], s['dnx'][1]], axis=1)
    dx = inv * (gd - xr * (jnp.sum(xr * gd, axis=-1, keepdims=True) / width))
    dx = dx + jnp.concatenate([s['bs'][0, chip], s['bs'][1, chip]], axis=1)
    de_ref[...] = jnp.where(core == 0, dx[:rows_e], dx[rows_e:])[:, :width]

    ag_o.finish()
    unpack(s['bo'], o_ref)


    for c in (r_e, r_i, r_w1, r_w2, r_dn):
        c.wait_send()
    for i in range(2):
        @pl.when(core == i)
        def _():
            d_give[i].wait_send()
    for x in (ag_n, rs_s, ag_s, rs_y, rs_d, ag_o):
        x.drain()


def rows_out(ids, o, de, dw1, dw2, out_ref, de_ref, dw1_ref, dw2_ref, buf, sem):
    _, vocab, half = o.shape
    copies = [pltpu.make_async_copy(src, dst, sem.at[i]) for i, (src, dst) in enumerate(
        ((dw1, dw1_ref), (dw2, dw2_ref), (de, de_ref), (buf.at[:half], out_ref.at[:half]), (buf.at[half:], out_ref.at[half:])))]
    for c in copies[:3]:
        c.start()
    mask = hot(ids[...], vocab)
    buf[:half] = dot(o[0], mask, 0, 0).astype(BF)
    copies[3].start()
    buf[half:] = dot(o[1], mask, 0, 0)[:buf.shape[0] - half].astype(BF)
    copies[4].start()
    for c in copies:
        c.wait()


def solution(mesh):
    tok_spec = P(('data', 'tensor'))
    row_spec = P(('data', 'tensor'), None)
    n_tensor = mesh.shape['tensor']
    chips = n_tensor // CORES
    side = math.isqrt(chips)
    assert side == 4 and side * side == chips

    def local_step(token_ids, emb_shard, norm_gain, w_up, w_down, grad_out):
        rows_e, width = emb_shard.shape
        tokens = token_ids.shape[0]
        f_loc = w_up.shape[1]
        f_chip = CORES * f_loc
        half = -(-width // 256) * 128
        rb = CORES * rows_e
        vocab = chips * rb
        vm = pltpu.VMEM
        dma = lambda *shape: pltpu.SemaphoreType.DMA(shape)
        scratch = dict(
            es=vm((2, rows_e, width), BF), gsrc=vm((width,), BF), ids=vm((2, 1, tokens), jnp.int32),
            w1s=vm((2, f_loc, width), BF), w2s=vm((2, f_loc, width), BF), dt=vm((2, half, tokens), BF), dg=vm((half, tokens), BF),
            e24=vm((rb, 2 * half), F32), w1p=vm((2, f_chip, half), BF), w2p=vm((2, f_chip, half), BF),
            bn=vm((2, chips, 2 * rb, half // 2), BF), bo=vm((2, chips, 2 * rb, half // 2), BF),
            bs=vm((2, chips, rb, half), F32), sp=vm((6, vocab, half), BF),
            n=vm((2, vocab, half), BF),
            gs=vm((chips, rb, half), F32), gy=vm((chips, rb, half), F32), gd=vm((chips, rb, half), F32),
            lay=vm((3, 4, rb, half), F32), ra=vm((3, 2, 4, rb, half), F32), rb=vm((3, 3, rb, half), F32),
            r=vm((3, 4, rb, half), F32),
            hid=vm((vocab, f_chip), BF), slope=vm((chips, rb, f_chip), F32), dh=vm((chips, rb, f_chip), F32),
            dnx=vm((2, rb, half), F32),
            lsem=dma(7), psem=dma(6), qsem=dma(6),
            gsem=dma(9), gd3=dma(2, 3), sr=dma(2, 9), gr=dma(2, 15),
        )
        names = list(scratch)

        def body(*refs):
            kernel(side, *refs[:10], dict(zip(names, refs[10:])))

        hbm = pl.BlockSpec(memory_space=pltpu.HBM)
        on_chip = pl.BlockSpec(memory_space=pltpu.VMEM)
        shapes = (
            jax.ShapeDtypeStruct((rows_e, width), F32),
            jax.ShapeDtypeStruct((f_loc, width), F32),
            jax.ShapeDtypeStruct((f_loc, width), F32),
        )
        ids_row = token_ids.reshape(1, tokens)
        done = pl.pallas_call(
            body,
            out_shape=(jax.ShapeDtypeStruct((2, vocab, half), BF),) + shapes,
            in_specs=[hbm] * 6,
            out_specs=(on_chip,) * 4,
            scratch_shapes=list(scratch.values()),
            compiler_params=pltpu.CompilerParams(
                collective_id=0, has_side_effects=True, vmem_limit_bytes=36 * 1024 * 1024),
            name='step',
        )(*(pltpu.with_memory_space_constraint(v, pltpu.HBM) for v in (
            ids_row, emb_shard, norm_gain, w_up.T, w_down, grad_out.T)))
        out_t, d_emb, dw1_t, d_w2 = pl.pallas_call(
            rows_out,
            out_shape=(jax.ShapeDtypeStruct((width, tokens), BF),) + shapes,
            in_specs=[on_chip] * 5,
            out_specs=(hbm,) * 4,
            scratch_shapes=[vm((width, tokens), BF), dma(5)],
            compiler_params=pltpu.CompilerParams(vmem_limit_bytes=16 * 1024 * 1024),
            name='rows_out',
        )(ids_row, *done)
        return out_t.T, d_emb, dw1_t.T, d_w2

    return jax.shard_map(
        local_step,
        mesh=mesh,
        in_specs=(tok_spec, P('tensor', None), P(None), P(None, 'tensor'), P('tensor', None), row_spec),
        out_specs=(row_spec, row_spec, P('data', 'tensor'), row_spec),
        check_vma=False,
    )
```

```python
import functools
import math

import jax
import jax.numpy as jnp
from jax import lax
from jax.experimental import pallas as pl
from jax.experimental.pallas import tpu as pltpu
from jax.sharding import PartitionSpec as P

EPS = 1e-6
BF = jnp.bfloat16
F32 = jnp.float32
CORES = 2
MESH = pl.DeviceIdType.MESH


def gelu_tanh(values):
    return jax.nn.gelu(values, approximate=True)


def parts(v):
    hi = v.astype(BF)
    r = v - hi.astype(F32)
    mid = r.astype(BF)
    lo = (r - mid.astype(F32)).astype(BF)
    return hi, mid, lo


def dot(a, b, ca, cb):
    return lax.dot_general(a, b, (((ca,), (cb,)), ((), ())), preferred_element_type=F32)


def pack(v):
    half = v.shape[1] // 2
    return jnp.concatenate([v[:, :half], v[:, half:]], axis=0).astype(BF)


def hot(ids_row, vocab):
    row = lax.broadcasted_iota(jnp.int32, (vocab, ids_row.shape[1]), 0)
    return jnp.where(row == ids_row, 1.0, 0.0).astype(BF)


class Ring:
    def __init__(self, side):
        me = lax.axis_index('tensor')
        self.side = side
        self.core = core = lax.rem(me, CORES)
        self.chip = chip = me // CORES
        x, y = lax.rem(chip, side), chip // side
        self.a = x * (1 - core) + y * core
        self.b = y * (1 - core) + x * core
        self.partner = {'tensor': me + 1 - 2 * core}

    def at(self, da, db):
        a = lax.rem(self.a + da, self.side)
        b = lax.rem(self.b + db, self.side)
        return a * (1 + (self.side - 1) * self.core) + b * (self.side - (self.side - 1) * self.core)

    def dev(self, da, db):
        return {'tensor': self.at(da, db) * CORES + self.core}


PLUS, MINUS = (2, 3), (1, 0)


class Scatter:
    def __init__(self, ring, g, relay, ra, rb, r, ssem, rsem):
        self.ring, self.g, self.relay, self.ra, self.rb, self.r = ring, g, relay, ra, rb, r
        self.ssem, self.rsem = ssem, rsem
        self.sent = []

    def copy(self, src, dst, i, dev):
        return pltpu.make_async_remote_copy(
            src_ref=src, dst_ref=dst, send_sem=self.ssem, recv_sem=self.rsem.at[i],
            device_id=dev, device_id_type=MESH)

    def c_relay(self, k):
        da = 1 if k in PLUS else 3
        return self.copy(self.g.at[self.ring.at(2, k)], self.relay.at[k], k, self.ring.dev(da, 0))

    def c_ring(self, k, plus):
        da = 1 if plus else 3
        j = 0 if plus else 1
        return self.copy(self.g.at[self.ring.at(da, k)], self.ra.at[j, k], 4 + k, self.ring.dev(da, 0))

    def c_b(self, k):
        return self.copy(self.r.at[k], self.rb.at[k - 1], 8, self.ring.dev(0, k))

    def go(self, c):
        c.start()
        self.sent.append(c)

    def relays(self, j):
        for kp, km in ((PLUS[j], MINUS[j]),):
            self.go(self.c_relay(kp))
            self.go(self.c_relay(km))

    def owns(self, j):
        for kp, km in ((MINUS[j], PLUS[j]),):
            self.go(self.c_ring(kp, True))
            self.go(self.c_ring(km, False))

    def middle(self, j):
        for kp, km in ((PLUS[j], MINUS[j]),):
            for k, plus in ((kp, True), (km, False)):
                self.c_relay(k).wait_recv()
                blk = self.ring.at(1 if plus else 3, k)
                self.g[blk] = self.g[blk] + self.relay[k]
                self.go(self.c_ring(k, plus))

    def short(self, *ks):
        for k in ks:
            self.arrived(2, 4 + k)
            self.r[k] = self.g[self.ring.at(0, k)] + self.ra[0, k] + self.ra[1, k]
            if k:
                self.go(self.c_b(k))

    def finish(self):
        self.arrived(3, 8)
        return self.r[0] + self.rb[0] + self.rb[2] + self.rb[1]

    def arrived(self, blocks, i):
        ref = self.g.at[pl.ds(0, blocks)]
        pltpu.make_async_copy(ref, ref, self.rsem.at[i]).wait()

    def drain(self):
        whole = self.g.at[pl.ds(0, len(self.sent))]
        pltpu.make_async_copy(whole, whole, self.ssem).wait()


FWD_P, FWD_M = (0, 2), (3, 1)


class Gather:
    def __init__(self, ring, buf, ssem, rsem, dsem, esem, direct=False):
        self.ring, self.buf, self.direct = ring, buf, direct
        self.ssem, self.rsem, self.dsem, self.esem = ssem, rsem, dsem, esem
        self.sent = []

    def copy(self, blk, i, dev):
        ref = self.buf.at[self.ring.core, blk]
        return pltpu.make_async_remote_copy(
            src_ref=ref, dst_ref=ref, send_sem=self.ssem, recv_sem=self.rsem.at[i],
            device_id=dev, device_id_type=MESH)

    def back(self, k):
        return (self.ring.side - k) % self.ring.side

    def go(self, c):
        c.start()
        self.sent.append(c)

    def over(self, blk, stage):
        ref = self.buf.at[self.ring.core, blk]
        pltpu.make_async_remote_copy(
            src_ref=ref, dst_ref=ref, send_sem=self.esem, recv_sem=self.dsem.at[stage],
            device_id=self.ring.partner, device_id_type=MESH).start()

    def both(self, k):
        blk = self.ring.at(0, self.back(k))
        self.go(self.copy(blk, k, self.ring.dev(1, 0)))
        self.go(self.copy(blk, 4 + k, self.ring.dev(3, 0)))
        if self.direct:
            self.go(self.copy(blk, 8 + k, self.ring.dev(2, 0)))

    def start(self):
        blk = self.ring.at(0, 0)
        for k in (2, 1, 3):
            self.go(self.copy(blk, 11 + k, self.ring.dev(0, k)))
        self.both(0)
        self.over(blk, 0)

    def first(self, *ks):
        for k in ks:
            blk = self.ring.at(0, self.back(k))
            self.copy(blk, 11 + k, self.ring.dev(0, k)).wait_recv()
            self.both(k)
            self.over(blk, 0)

    def middle(self, *ks):
        for k in ks:
            blk = self.ring.at(3, self.back(k))
            self.copy(blk, k, self.ring.dev(1, 0)).wait_recv()
            if k in FWD_P and not self.direct:
                self.go(self.copy(blk, 8 + k, self.ring.dev(1, 0)))
            self.over(blk, 1)
            blk = self.ring.at(1, self.back(k))
            self.copy(blk, 4 + k, self.ring.dev(3, 0)).wait_recv()
            if k in FWD_M and not self.direct:
                self.go(self.copy(blk, 8 + k, self.ring.dev(3, 0)))
            self.over(blk, 1)

    def last(self, *ks):
        for k in ks:
            blk = self.ring.at(2, self.back(k))
            self.copy(blk, 8 + k, self.ring.dev(1, 0)).wait_recv()
            self.over(blk, 2)

    def passed(self, stage):
        ref = self.buf.at[1 - self.ring.core, pl.ds(0, (4, 8, 4)[stage])]
        pltpu.make_async_copy(ref, ref, self.dsem.at[stage]).wait()

    def finish(self):
        for stage in range(3):
            self.passed(stage)

    def drain(self):
        ref = self.buf.at[self.ring.core]
        pltpu.make_async_copy(ref, ref, self.esem).wait()
        ref = self.buf.at[0, pl.ds(0, len(self.sent))]
        pltpu.make_async_copy(ref, ref, self.ssem).wait()


def kernel(side, ids_in, e_in, g_in, w1_in, w2_in, d_in, o_ref, de_ref, dw1_ref, dw2_ref, s):
    ring = Ring(side)
    core, chip, partner = ring.core, ring.chip, ring.partner
    chips = side * side
    rows_e, width = e_in.shape
    f_loc = w1_in.shape[0]
    f_chip = CORES * f_loc
    half = s['w1p'].shape[2]
    rest = width - half
    rb = s['gs'].shape[1]
    vocab = chips * rb

    def local(src, dst, i):
        return pltpu.make_async_copy(src, dst, s['lsem'].at[i])

    def pair(src, dst, i):
        return pltpu.make_async_remote_copy(
            src_ref=src, dst_ref=dst, send_sem=s['psem'].at[i], recv_sem=s['qsem'].at[i],
            device_id=partner, device_id_type=MESH)

    c_e = local(e_in, s['es'].at[core], 0)
    c_g = local(g_in, s['gsrc'], 1)
    c_i = local(ids_in, s['ids'].at[core], 2)
    c_w1 = local(w1_in, s['w1s'].at[core], 3)
    c_w2 = local(w2_in, s['w2s'].at[core], 4)
    d_own = (local(d_in.at[:half], s['dt'].at[0], 5),
             local(d_in.at[half:], s['dt'].at[0, :rest], 5))
    r_e = pair(s['es'].at[core], s['es'].at[core], 0)
    r_i = pair(s['ids'].at[core], s['ids'].at[core], 1)
    r_w1 = pair(w1_in, s['w1s'].at[core], 2)
    r_w2 = pair(w2_in, s['w2s'].at[core], 3)
    d_load = (local(d_in.at[half:], s['dg'].at[:rest], 6),
              local(d_in.at[:half], s['dg'], 6))
    d_give = (pair(s['dg'].at[:rest], s['dt'].at[1, :rest], 4),
              pair(s['dg'], s['dt'].at[1], 4))

    c_e.start()
    for i in range(2):
        @pl.when(core == i)
        def _():
            d_load[i].start()
    c_g.start()
    c_i.start()

    @pl.when(core == 1)
    def _():
        for j in range(2):
            s['dt'][j, rest:, :] = jnp.zeros((half - rest, s['dt'].shape[2]), BF)

    barrier = pltpu.get_barrier_semaphore()
    peers = [partner, ring.dev(1, 0), ring.dev(3, 0)] + [ring.dev(0, k) for k in (1, 2, 3)]
    for p in peers:
        pl.semaphore_signal(barrier, inc=1, device_id=p, device_id_type=MESH)
    for i in range(2):
        @pl.when(core == i)
        def _():
            d_own[i].start()
    c_w1.start()
    c_w2.start()
    pl.semaphore_wait(barrier, len(peers))

    c_e.wait()
    r_e.start()
    for i in range(2):
        @pl.when(core == i)
        def _():
            d_load[i].wait()
            d_give[i].start()
    c_i.wait()
    r_i.start()
    r_w1.start()
    r_w2.start()

    def wide(v):
        return jnp.concatenate([v, jnp.zeros((v.shape[0], 2 * half - width), F32)], axis=1)

    c_g.wait()
    r_e.wait_recv()
    gain = wide(s['gsrc'][...].astype(F32).reshape(1, width))
    for i in range(2):
        s['e24'][i * rows_e:(i + 1) * rows_e, :] = wide(s['es'][i].astype(F32))

    def inv_rms(x):
        return lax.rsqrt(jnp.sum(x * x, axis=-1, keepdims=True) / width + EPS)

    def mine(v):
        return jnp.where(core == 0, v[:, :half], v[:, half:])

    x24 = s['e24'][...]
    ag_n = Gather(ring, s['bn'], s['gsem'].at[3], s['gr'].at[0], s['gd3'].at[0], s['gsem'].at[6])
    s['bn'][core, chip] = pack(mine(x24 * inv_rms(x24) * gain))
    ag_n.start()

    for i in range(2):
        @pl.when(core == i)
        def _():
            d_own[i].wait()
    def s_rows(da, src):
        blks = [ring.at(da, k) for k in range(side)]
        row = jnp.concatenate([rb * blk + lax.broadcasted_iota(jnp.int32, (rb, s['dt'].shape[2]), 0) for blk in blks], axis=0)
        pick = jnp.where(row == s['ids'][core if src == 0 else 1 - core], 1.0, 0.0).astype(BF)
        d = dot(pick, s['dt'][src], 1, 1)
        for i, blk in enumerate(blks):
            v = d[i * rb:(i + 1) * rb]
            s['gs'][blk] = v if src == 0 else s['gs'][blk] + v

    s_rows(2, 0)
    r_i.wait_recv()
    for i in range(2):
        @pl.when(core == i)
        def _():
            d_give[1 - i].wait_recv()

    s_rows(2, 1)
    rs_s = Scatter(ring, s['gs'], s['lay'].at[0], s['ra'].at[0], s['rb'].at[0], s['r'].at[0], s['gsem'].at[0], s['sr'].at[0])
    rs_s.relays(0)
    rs_s.relays(1)
    for da in (1, 3):
        for src in range(2):
            s_rows(da, src)
    rs_s.owns(0)
    rs_s.owns(1)
    for src in range(2):
        s_rows(0, src)


    def tall(v):
        return jnp.concatenate(parts(v), axis=0)

    def short(v):
        n = v.shape[0] // 3
        return v[2 * n:] + v[n:2 * n] + v[:n]

    def dh_add(h, blks):
        v = jnp.concatenate([s['bs'][h, blk] for blk in blks], axis=0)
        d = short(dot(tall(v), s['w2p'][h], 1, 1))
        for i, blk in enumerate(blks):
            s['dh'][blk] = s['dh'][blk] + d[i * rb:(i + 1) * rb]

    def line(da):
        return [ring.at(da, k) for k in range(side)]

    def cross(db):
        return [ring.at(k, db) for k in range(side)]

    def dn_rows(da):
        blks = line(da)
        du = [s['dh'][blk] * s['slope'][blk] for blk in blks]
        for blk, v in zip(blks, du):
            s['dh'][blk] = v
        d = short(dot(tall(jnp.concatenate(du, axis=0)), s['w1p'][core], 1, 0))
        for i, blk in enumerate(blks):
            s['gd'][blk] = d[i * rb:(i + 1) * rb]

    def own(v):
        return jnp.where(core == 0, v[:, :f_loc], v[:, f_loc:])

    c_w1.wait()
    c_w2.wait()
    r_w1.wait_recv()
    r_w2.wait_recv()
    for w_src, w_dst in (('w1s', 'w1p'), ('w2s', 'w2p')):
        for i in range(2):
            rows = slice(i * f_loc, (i + 1) * f_loc)
            s[w_dst][0, rows, :] = s[w_src][i, :, :half]
            s[w_dst][1, rows, :] = jnp.concatenate(
                [s[w_src][i, :, half:], jnp.zeros((f_loc, half - rest), BF)], axis=1)

    ag_n.first(1)
    ag_n.first(3)
    ag_n.first(2)
    rs_s.middle(0)
    rs_s.middle(1)
    ag_n.middle(0)
    ag_n.middle(1)
    ag_n.middle(3)
    ag_n.middle(2)
    rs_s.short(2)
    rs_s.short(3)
    rs_s.short(1)
    rs_s.short(0)
    ag_n.last(0)
    ag_n.last(3)
    ag_n.last(1)
    ag_n.last(2)
    ag_n.finish()

    def unpack(buf, dst):
        q = half // 2
        for h in range(2):
            v = buf[h].astype(F32)
            dst[h, :, :q] = v[:, :rb].reshape(vocab, q).astype(BF)
            dst[h, :, q:] = v[:, rb:].reshape(vocab, q).astype(BF)

    unpack(s['bn'], s['n'])
    pre = (dot(s['n'][0], s['w1p'][0], 1, 1) + dot(s['n'][1], s['w1p'][1], 1, 1)).astype(BF)
    pre_f = pre.astype(F32)
    act, gelu_back = jax.vjp(gelu_tanh, pre_f)
    hid = act.astype(BF)
    s['hid'][...] = hid
    s['slope'][...] = gelu_back(jnp.ones_like(pre_f))[0].reshape(chips, rb, f_chip)
    s['dh'][...] = jnp.zeros((chips, rb, f_chip), F32)
    s['gy'][...] = dot(hid, s['w2p'][core], 1, 0).reshape(chips, rb, half)

    ag_s = Gather(ring, s['bs'], s['gsem'].at[4], s['gr'].at[1], s['gd3'].at[1], s['gsem'].at[7])
    s['bs'][core, chip] = rs_s.finish()
    ag_s.start()
    rs_y = Scatter(ring, s['gy'], s['lay'].at[1], s['ra'].at[1], s['rb'].at[1], s['r'].at[1], s['gsem'].at[1], s['sr'].at[1])
    rs_y.relays(0)
    rs_y.relays(1)
    rs_y.owns(0)
    rs_y.owns(1)
    ag_s.first(1)
    ag_s.first(3)
    ag_s.first(2)
    ag_s.middle(0)
    dh_add(core, line(0))
    rs_y.middle(0)
    rs_y.middle(1)
    ag_s.middle(1)
    ag_s.middle(3)
    ag_s.middle(2)
    dh_add(core, line(1) + line(3))
    ag_s.passed(0)
    dh_add(1 - core, cross(0))
    rs_y.short(2)
    rs_y.short(1)
    rs_y.short(3)
    rs_y.short(0)
    ag_s.passed(1)
    dh_add(1 - core, cross(1) + cross(3))
    ag_s.last(0)
    ag_s.last(3)
    ag_s.last(1)
    ag_s.last(2)
    dh_add(core, line(2))
    ag_s.passed(2)
    dh_add(1 - core, cross(2))
    rs_d = Scatter(ring, s['gd'], s['lay'].at[2], s['ra'].at[2], s['rb'].at[2], s['r'].at[2], s['gsem'].at[2], s['sr'].at[0])
    dn_rows(2)
    rs_d.relays(0)
    rs_d.relays(1)
    dn_rows(1)
    dn_rows(3)
    rs_d.owns(0)
    rs_d.owns(1)
    dn_rows(0)
    ag_o = Gather(ring, s['bo'], s['gsem'].at[5], s['gr'].at[0], s['gd3'].at[0], s['gsem'].at[8])
    s['bo'][core, chip] = pack(mine(s['e24'][...]) + rs_y.finish())
    ag_o.start()
    for i in range(2):
        for j, p in enumerate(parts(s['bs'][i].reshape(vocab, half))):
            s['sp'][3 * i + j] = p

    hid_own = own(s['hid'][...].astype(F32)).astype(BF)
    for i in range(2):
        acc = jnp.zeros((f_loc, half), F32)
        for j in (2, 1, 0):
            acc = acc + dot(hid_own, s['sp'][3 * i + j], 0, 0)
        if i == 0:
            dw2_ref[:, :half] = acc
        else:
            dw2_ref[:, half:] = acc[:, :rest]

    rs_d.middle(0)
    rs_d.middle(1)
    ag_o.first(1)
    ag_o.first(3)
    ag_o.first(2)
    ag_o.middle(0)
    rs_d.short(2)
    rs_d.short(1)
    rs_d.short(3)
    du_own = parts(own(s['dh'][...].reshape(vocab, f_chip)))
    for i in range(2):
        acc = jnp.zeros((f_loc, half), F32)
        for p in du_own[::-1]:
            acc = acc + dot(p, s['n'][i], 0, 0)
        if i == 0:
            dw1_ref[:, :half] = acc
        else:
            dw1_ref[:, half:] = acc[:, :rest]

    rs_d.short(0)
    ag_o.middle(1)
    ag_o.middle(3)
    ag_o.middle(2)
    s['dnx'][core] = rs_d.finish()
    r_dn = pair(s['dnx'].at[core], s['dnx'].at[core], 5)
    r_dn.start()
    ag_o.last(0)
    ag_o.last(3)
    ag_o.last(1)
    ag_o.last(2)
    pair(s['dnx'].at[1 - core], s['dnx'].at[1 - core], 5).wait_recv()
    inv = inv_rms(s['e24'][...])
    xr = s['e24'][...] * inv
    gd = gain * jnp.concatenate([s['dnx'][0], s['dnx'][1]], axis=1)
    dx = inv * (gd - xr * (jnp.sum(xr * gd, axis=-1, keepdims=True) / width))
    dx = dx + jnp.concatenate([s['bs'][0, chip], s['bs'][1, chip]], axis=1)
    de_ref[...] = jnp.where(core == 0, dx[:rows_e], dx[rows_e:])[:, :width]

    ag_o.finish()
    unpack(s['bo'], o_ref)


    for c in (r_e, r_i, r_w1, r_w2, r_dn):
        c.wait_send()
    for i in range(2):
        @pl.when(core == i)
        def _():
            d_give[i].wait_send()
    for x in (ag_n, rs_s, ag_s, rs_y, rs_d, ag_o):
        x.drain()


def rows_out(ids, o, de, dw1, dw2, out_ref, de_ref, dw1_ref, dw2_ref, buf, sem):
    _, vocab, half = o.shape
    copies = [pltpu.make_async_copy(src, dst, sem.at[i]) for i, (src, dst) in enumerate(
        ((dw1, dw1_ref), (dw2, dw2_ref), (de, de_ref), (buf.at[:half], out_ref.at[:half]), (buf.at[half:], out_ref.at[half:])))]
    for c in copies[:3]:
        c.start()
    mask = hot(ids[...], vocab)
    buf[:half] = dot(o[0], mask, 0, 0).astype(BF)
    copies[3].start()
    buf[half:] = dot(o[1], mask, 0, 0)[:buf.shape[0] - half].astype(BF)
    copies[4].start()
    for c in copies:
        c.wait()


def solution(mesh):
    tok_spec = P(('data', 'tensor'))
    row_spec = P(('data', 'tensor'), None)
    n_tensor = mesh.shape['tensor']
    chips = n_tensor // CORES
    side = math.isqrt(chips)
    assert side == 4 and side * side == chips

    def local_step(token_ids, emb_shard, norm_gain, w_up, w_down, grad_out):
        rows_e, width = emb_shard.shape
        tokens = token_ids.shape[0]
        f_loc = w_up.shape[1]
        f_chip = CORES * f_loc
        half = -(-width // 256) * 128
        rb = CORES * rows_e
        vocab = chips * rb
        vm = pltpu.VMEM
        dma = lambda *shape: pltpu.SemaphoreType.DMA(shape)
        scratch = dict(
            es=vm((2, rows_e, width), BF), gsrc=vm((width,), BF), ids=vm((2, 1, tokens), jnp.int32),
            w1s=vm((2, f_loc, width), BF), w2s=vm((2, f_loc, width), BF), dt=vm((2, half, tokens), BF), dg=vm((half, tokens), BF),
            e24=vm((rb, 2 * half), F32), w1p=vm((2, f_chip, half), BF), w2p=vm((2, f_chip, half), BF),
            bn=vm((2, chips, 2 * rb, half // 2), BF), bo=vm((2, chips, 2 * rb, half // 2), BF),
            bs=vm((2, chips, rb, half), F32), sp=vm((6, vocab, half), BF),
            n=vm((2, vocab, half), BF),
            gs=vm((chips, rb, half), F32), gy=vm((chips, rb, half), F32), gd=vm((chips, rb, half), F32),
            lay=vm((3, 4, rb, half), F32), ra=vm((3, 2, 4, rb, half), F32), rb=vm((3, 3, rb, half), F32),
            r=vm((3, 4, rb, half), F32),
            hid=vm((vocab, f_chip), BF), slope=vm((chips, rb, f_chip), F32), dh=vm((chips, rb, f_chip), F32),
            dnx=vm((2, rb, half), F32),
            lsem=dma(7), psem=dma(6), qsem=dma(6),
            gsem=dma(9), gd3=dma(2, 3), sr=dma(2, 9), gr=dma(2, 15),
        )
        names = list(scratch)

        def body(*refs):
            kernel(side, *refs[:10], dict(zip(names, refs[10:])))

        hbm = pl.BlockSpec(memory_space=pltpu.HBM)
        on_chip = pl.BlockSpec(memory_space=pltpu.VMEM)
        shapes = (
            jax.ShapeDtypeStruct((rows_e, width), F32),
            jax.ShapeDtypeStruct((f_loc, width), F32),
            jax.ShapeDtypeStruct((f_loc, width), F32),
        )
        ids_row = token_ids.reshape(1, tokens)
        done = pl.pallas_call(
            body,
            out_shape=(jax.ShapeDtypeStruct((2, vocab, half), BF),) + shapes,
            in_specs=[hbm] * 6,
            out_specs=(on_chip,) * 4,
            scratch_shapes=list(scratch.values()),
            compiler_params=pltpu.CompilerParams(
                collective_id=0, has_side_effects=True, vmem_limit_bytes=36 * 1024 * 1024),
            name='step',
        )(*(pltpu.with_memory_space_constraint(v, pltpu.HBM) for v in (
            ids_row, emb_shard, norm_gain, w_up.T, w_down, grad_out.T)))
        out_t, d_emb, dw1_t, d_w2 = pl.pallas_call(
            rows_out,
            out_shape=(jax.ShapeDtypeStruct((width, tokens), BF),) + shapes,
            in_specs=[on_chip] * 5,
            out_specs=(hbm,) * 4,
            scratch_shapes=[vm((width, tokens), BF), dma(5)],
            compiler_params=pltpu.CompilerParams(vmem_limit_bytes=16 * 1024 * 1024),
            name='rows_out',
        )(ids_row, *done)
        return out_t.T, d_emb, dw1_t.T, d_w2

    return jax.shard_map(
        local_step,
        mesh=mesh,
        in_specs=(tok_spec, P('tensor', None), P(None), P(None, 'tensor'), P('tensor', None), row_spec),
        out_specs=(row_spec, row_spec, P('data', 'tensor'), row_spec),
        check_vma=False,
    )
```

```python
import functools
import math

import jax
import jax.numpy as jnp
from jax import lax
from jax.experimental import pallas as pl
from jax.experimental.pallas import tpu as pltpu
from jax.sharding import PartitionSpec as P

EPS = 1e-6
BF = jnp.bfloat16
F32 = jnp.float32
CORES = 2
MESH = pl.DeviceIdType.MESH


def gelu_tanh(values):
    return jax.nn.gelu(values, approximate=True)


def parts(v):
    hi = v.astype(BF)
    r = v - hi.astype(F32)
    mid = r.astype(BF)
    lo = (r - mid.astype(F32)).astype(BF)
    return hi, mid, lo


def dot(a, b, ca, cb):
    return lax.dot_general(a, b, (((ca,), (cb,)), ((), ())), preferred_element_type=F32)


def pack(v):
    half = v.shape[1] // 2
    return jnp.concatenate([v[:, :half], v[:, half:]], axis=0).astype(BF)


def hot(ids_row, vocab):
    row = lax.broadcasted_iota(jnp.int32, (vocab, ids_row.shape[1]), 0)
    return jnp.where(row == ids_row, 1.0, 0.0).astype(BF)


class Ring:
    def __init__(self, side):
        me = lax.axis_index('tensor')
        self.side = side
        self.core = core = lax.rem(me, CORES)
        self.chip = chip = me // CORES
        x, y = lax.rem(chip, side), chip // side
        self.a = x * (1 - core) + y * core
        self.b = y * (1 - core) + x * core
        self.partner = {'tensor': me + 1 - 2 * core}

    def at(self, da, db):
        a = lax.rem(self.a + da, self.side)
        b = lax.rem(self.b + db, self.side)
        return a * (1 + (self.side - 1) * self.core) + b * (self.side - (self.side - 1) * self.core)

    def dev(self, da, db):
        return {'tensor': self.at(da, db) * CORES + self.core}


PLUS, MINUS = (2, 3), (1, 0)


class Scatter:
    def __init__(self, ring, g, relay, ra, rb, r, ssem, rsem):
        self.ring, self.g, self.relay, self.ra, self.rb, self.r = ring, g, relay, ra, rb, r
        self.ssem, self.rsem = ssem, rsem
        self.sent = []

    def copy(self, src, dst, i, dev):
        return pltpu.make_async_remote_copy(
            src_ref=src, dst_ref=dst, send_sem=self.ssem, recv_sem=self.rsem.at[i],
            device_id=dev, device_id_type=MESH)

    def c_relay(self, k):
        da = 1 if k in PLUS else 3
        return self.copy(self.g.at[self.ring.at(2, k)], self.relay.at[k], k, self.ring.dev(da, 0))

    def c_ring(self, k, plus):
        da = 1 if plus else 3
        j = 0 if plus else 1
        return self.copy(self.g.at[self.ring.at(da, k)], self.ra.at[j, k], 4 + k, self.ring.dev(da, 0))

    def c_b(self, k):
        return self.copy(self.r.at[k], self.rb.at[k - 1], 8, self.ring.dev(0, k))

    def go(self, c):
        c.start()
        self.sent.append(c)

    def relays(self, j):
        for kp, km in ((PLUS[j], MINUS[j]),):
            self.go(self.c_relay(kp))
            self.go(self.c_relay(km))

    def owns(self, j):
        for kp, km in ((MINUS[j], PLUS[j]),):
            self.go(self.c_ring(kp, True))
            self.go(self.c_ring(km, False))

    def middle(self, j):
        for kp, km in ((PLUS[j], MINUS[j]),):
            for k, plus in ((kp, True), (km, False)):
                self.c_relay(k).wait_recv()
                blk = self.ring.at(1 if plus else 3, k)
                self.g[blk] = self.g[blk] + self.relay[k]
                self.go(self.c_ring(k, plus))

    def short(self, *ks):
        for k in ks:
            self.arrived(2, 4 + k)
            self.r[k] = self.g[self.ring.at(0, k)] + self.ra[0, k] + self.ra[1, k]
            if k:
                self.go(self.c_b(k))

    def finish(self):
        self.arrived(3, 8)
        return self.r[0] + self.rb[0] + self.rb[2] + self.rb[1]

    def arrived(self, blocks, i):
        ref = self.g.at[pl.ds(0, blocks)]
        pltpu.make_async_copy(ref, ref, self.rsem.at[i]).wait()

    def drain(self):
        whole = self.g.at[pl.ds(0, len(self.sent))]
        pltpu.make_async_copy(whole, whole, self.ssem).wait()


FWD_P, FWD_M = (0, 2), (3, 1)


class Gather:
    def __init__(self, ring, buf, ssem, rsem, dsem, esem, direct=False):
        self.ring, self.buf, self.direct = ring, buf, direct
        self.ssem, self.rsem, self.dsem, self.esem = ssem, rsem, dsem, esem
        self.sent = []

    def copy(self, blk, i, dev):
        ref = self.buf.at[self.ring.core, blk]
        return pltpu.make_async_remote_copy(
            src_ref=ref, dst_ref=ref, send_sem=self.ssem, recv_sem=self.rsem.at[i],
            device_id=dev, device_id_type=MESH)

    def back(self, k):
        return (self.ring.side - k) % self.ring.side

    def go(self, c):
        c.start()
        self.sent.append(c)

    def over(self, blk, stage):
        ref = self.buf.at[self.ring.core, blk]
        pltpu.make_async_remote_copy(
            src_ref=ref, dst_ref=ref, send_sem=self.esem, recv_sem=self.dsem.at[stage],
            device_id=self.ring.partner, device_id_type=MESH).start()

    def both(self, k):
        blk = self.ring.at(0, self.back(k))
        self.go(self.copy(blk, k, self.ring.dev(1, 0)))
        self.go(self.copy(blk, 4 + k, self.ring.dev(3, 0)))
        if self.direct:
            self.go(self.copy(blk, 8 + k, self.ring.dev(2, 0)))

    def start(self):
        blk = self.ring.at(0, 0)
        for k in (2, 1, 3):
            self.go(self.copy(blk, 11 + k, self.ring.dev(0, k)))
        self.both(0)
        self.over(blk, 0)

    def first(self, *ks):
        for k in ks:
            blk = self.ring.at(0, self.back(k))
            self.copy(blk, 11 + k, self.ring.dev(0, k)).wait_recv()
            self.both(k)
            self.over(blk, 0)

    def middle(self, *ks):
        for k in ks:
            blk = self.ring.at(3, self.back(k))
            self.copy(blk, k, self.ring.dev(1, 0)).wait_recv()
            if k in FWD_P and not self.direct:
                self.go(self.copy(blk, 8 + k, self.ring.dev(1, 0)))
            self.over(blk, 1)
            blk = self.ring.at(1, self.back(k))
            self.copy(blk, 4 + k, self.ring.dev(3, 0)).wait_recv()
            if k in FWD_M and not self.direct:
                self.go(self.copy(blk, 8 + k, self.ring.dev(3, 0)))
            self.over(blk, 1)

    def last(self, *ks):
        for k in ks:
            blk = self.ring.at(2, self.back(k))
            self.copy(blk, 8 + k, self.ring.dev(1, 0)).wait_recv()
            self.over(blk, 2)

    def passed(self, stage):
        ref = self.buf.at[1 - self.ring.core, pl.ds(0, (4, 8, 4)[stage])]
        pltpu.make_async_copy(ref, ref, self.dsem.at[stage]).wait()

    def finish(self):
        for stage in range(3):
            self.passed(stage)

    def drain(self):
        ref = self.buf.at[self.ring.core]
        pltpu.make_async_copy(ref, ref, self.esem).wait()
        ref = self.buf.at[0, pl.ds(0, len(self.sent))]
        pltpu.make_async_copy(ref, ref, self.ssem).wait()


def kernel(side, ids_in, e_in, g_in, w1_in, w2_in, d_in, o_ref, de_ref, dw1_ref, dw2_ref, s):
    ring = Ring(side)
    core, chip, partner = ring.core, ring.chip, ring.partner
    chips = side * side
    rows_e, width = e_in.shape
    f_loc = w1_in.shape[0]
    f_chip = CORES * f_loc
    half = s['w1p'].shape[2]
    rest = width - half
    rb = s['gs'].shape[1]
    vocab = chips * rb

    def local(src, dst, i):
        return pltpu.make_async_copy(src, dst, s['lsem'].at[i])

    def pair(src, dst, i):
        return pltpu.make_async_remote_copy(
            src_ref=src, dst_ref=dst, send_sem=s['psem'].at[i], recv_sem=s['qsem'].at[i],
            device_id=partner, device_id_type=MESH)

    c_e = local(e_in, s['es'].at[core], 0)
    c_g = local(g_in, s['gsrc'], 1)
    c_i = local(ids_in, s['ids'].at[core], 2)
    c_w1 = local(w1_in, s['w1s'].at[core], 3)
    c_w2 = local(w2_in, s['w2s'].at[core], 4)
    d_own = (local(d_in.at[:half], s['dt'].at[0], 5),
             local(d_in.at[half:], s['dt'].at[0, :rest], 5))
    r_e = pair(s['es'].at[core], s['es'].at[core], 0)
    r_i = pair(s['ids'].at[core], s['ids'].at[core], 1)
    r_w1 = pair(w1_in, s['w1s'].at[core], 2)
    r_w2 = pair(w2_in, s['w2s'].at[core], 3)
    d_load = (local(d_in.at[half:], s['dg'].at[:rest], 6),
              local(d_in.at[:half], s['dg'], 6))
    d_give = (pair(s['dg'].at[:rest], s['dt'].at[1, :rest], 4),
              pair(s['dg'], s['dt'].at[1], 4))

    c_e.start()
    for i in range(2):
        @pl.when(core == i)
        def _():
            d_load[i].start()
    c_g.start()
    c_i.start()

    @pl.when(core == 1)
    def _():
        for j in range(2):
            s['dt'][j, rest:, :] = jnp.zeros((half - rest, s['dt'].shape[2]), BF)

    barrier = pltpu.get_barrier_semaphore()
    peers = [partner, ring.dev(1, 0), ring.dev(3, 0)] + [ring.dev(0, k) for k in (1, 2, 3)]
    for p in peers:
        pl.semaphore_signal(barrier, inc=1, device_id=p, device_id_type=MESH)
    for i in range(2):
        @pl.when(core == i)
        def _():
            d_own[i].start()
    c_w1.start()
    c_w2.start()
    pl.semaphore_wait(barrier, len(peers))

    c_e.wait()
    r_e.start()
    for i in range(2):
        @pl.when(core == i)
        def _():
            d_load[i].wait()
            d_give[i].start()
    c_i.wait()
    r_i.start()
    r_w1.start()
    r_w2.start()

    def wide(v):
        return jnp.concatenate([v, jnp.zeros((v.shape[0], 2 * half - width), F32)], axis=1)

    c_g.wait()
    r_e.wait_recv()
    gain = wide(s['gsrc'][...].astype(F32).reshape(1, width))
    for i in range(2):
        s['e24'][i * rows_e:(i + 1) * rows_e, :] = wide(s['es'][i].astype(F32))

    def inv_rms(x):
        return lax.rsqrt(jnp.sum(x * x, axis=-1, keepdims=True) / width + EPS)

    def mine(v):
        return jnp.where(core == 0, v[:, :half], v[:, half:])

    x24 = s['e24'][...]
    ag_n = Gather(ring, s['bn'], s['gsem'].at[3], s['gr'].at[0], s['gd3'].at[0], s['gsem'].at[6])
    s['bn'][core, chip] = pack(mine(x24 * inv_rms(x24) * gain))
    ag_n.start()

    for i in range(2):
        @pl.when(core == i)
        def _():
            d_own[i].wait()
    def s_rows(da, src):
        blks = [ring.at(da, k) for k in range(side)]
        row = jnp.concatenate([rb * blk + lax.broadcasted_iota(jnp.int32, (rb, s['dt'].shape[2]), 0) for blk in blks], axis=0)
        pick = jnp.where(row == s['ids'][core if src == 0 else 1 - core], 1.0, 0.0).astype(BF)
        d = dot(pick, s['dt'][src], 1, 1)
        for i, blk in enumerate(blks):
            v = d[i * rb:(i + 1) * rb]
            s['gs'][blk] = v if src == 0 else s['gs'][blk] + v

    s_rows(2, 0)
    r_i.wait_recv()
    for i in range(2):
        @pl.when(core == i)
        def _():
            d_give[1 - i].wait_recv()

    s_rows(2, 1)
    rs_s = Scatter(ring, s['gs'], s['lay'].at[0], s['ra'].at[0], s['rb'].at[0], s['r'].at[0], s['gsem'].at[0], s['sr'].at[0])
    rs_s.relays(0)
    rs_s.relays(1)
    for da in (1, 3):
        for src in range(2):
            s_rows(da, src)
    rs_s.owns(0)
    rs_s.owns(1)
    for src in range(2):
        s_rows(0, src)


    def tall(v):
        return jnp.concatenate(parts(v), axis=0)

    def short(v):
        n = v.shape[0] // 3
        return v[2 * n:] + v[n:2 * n] + v[:n]

    def dh_add(h, blks):
        v = jnp.concatenate([s['bs'][h, blk] for blk in blks], axis=0)
        d = short(dot(tall(v), s['w2p'][h], 1, 1))
        for i, blk in enumerate(blks):
            s['dh'][blk] = s['dh'][blk] + d[i * rb:(i + 1) * rb]

    def line(da):
        return [ring.at(da, k) for k in range(side)]

    def cross(db):
        return [ring.at(k, db) for k in range(side)]

    def dn_rows(da):
        blks = line(da)
        du = [s['dh'][blk] * s['slope'][blk] for blk in blks]
        for blk, v in zip(blks, du):
            s['dh'][blk] = v
        d = short(dot(tall(jnp.concatenate(du, axis=0)), s['w1p'][core], 1, 0))
        for i, blk in enumerate(blks):
            s['gd'][blk] = d[i * rb:(i + 1) * rb]

    def own(v):
        return jnp.where(core == 0, v[:, :f_loc], v[:, f_loc:])

    c_w1.wait()
    c_w2.wait()
    r_w1.wait_recv()
    r_w2.wait_recv()
    for w_src, w_dst in (('w1s', 'w1p'), ('w2s', 'w2p')):
        for i in range(2):
            rows = slice(i * f_loc, (i + 1) * f_loc)
            s[w_dst][0, rows, :] = s[w_src][i, :, :half]
            s[w_dst][1, rows, :] = jnp.concatenate(
                [s[w_src][i, :, half:], jnp.zeros((f_loc, half - rest), BF)], axis=1)

    ag_n.first(1)
    ag_n.first(3)
    ag_n.first(2)
    rs_s.middle(0)
    rs_s.middle(1)
    ag_n.middle(0)
    ag_n.middle(1)
    ag_n.middle(3)
    ag_n.middle(2)
    rs_s.short(2)
    rs_s.short(3)
    rs_s.short(1)
    rs_s.short(0)
    ag_n.last(0)
    ag_n.last(3)
    ag_n.last(1)
    ag_n.last(2)
    ag_n.finish()

    def unpack(buf, dst):
        q = half // 2
        for h in range(2):
            v = buf[h].astype(F32)
            dst[h, :, :q] = v[:, :rb].reshape(vocab, q).astype(BF)
            dst[h, :, q:] = v[:, rb:].reshape(vocab, q).astype(BF)

    unpack(s['bn'], s['n'])
    pre = (dot(s['n'][0], s['w1p'][0], 1, 1) + dot(s['n'][1], s['w1p'][1], 1, 1)).astype(BF)
    pre_f = pre.astype(F32)
    act, gelu_back = jax.vjp(gelu_tanh, pre_f)
    hid = act.astype(BF)
    s['hid'][...] = hid
    s['slope'][...] = gelu_back(jnp.ones_like(pre_f))[0].reshape(chips, rb, f_chip)
    s['dh'][...] = jnp.zeros((chips, rb, f_chip), F32)
    s['gy'][...] = dot(hid, s['w2p'][core], 1, 0).reshape(chips, rb, half)

    ag_s = Gather(ring, s['bs'], s['gsem'].at[4], s['gr'].at[1], s['gd3'].at[1], s['gsem'].at[7])
    s['bs'][core, chip] = rs_s.finish()
    ag_s.start()
    rs_y = Scatter(ring, s['gy'], s['lay'].at[1], s['ra'].at[1], s['rb'].at[1], s['r'].at[1], s['gsem'].at[1], s['sr'].at[1])
    rs_y.relays(0)
    rs_y.relays(1)
    rs_y.owns(0)
    rs_y.owns(1)
    ag_s.first(1)
    ag_s.first(3)
    ag_s.first(2)
    ag_s.middle(0)
    rs_y.middle(0)
    dh_add(core, line(0))
    rs_y.middle(1)
    ag_s.middle(1)
    ag_s.middle(3)
    ag_s.middle(2)
    dh_add(core, line(1) + line(3))
    ag_s.passed(0)
    dh_add(1 - core, cross(0))
    rs_y.short(2)
    rs_y.short(1)
    rs_y.short(3)
    rs_y.short(0)
    ag_s.passed(1)
    dh_add(1 - core, cross(1) + cross(3))
    ag_s.last(0)
    ag_s.last(3)
    ag_s.last(1)
    ag_s.last(2)
    dh_add(core, line(2))
    ag_s.passed(2)
    dh_add(1 - core, cross(2))
    rs_d = Scatter(ring, s['gd'], s['lay'].at[2], s['ra'].at[2], s['rb'].at[2], s['r'].at[2], s['gsem'].at[2], s['sr'].at[0])
    dn_rows(2)
    rs_d.relays(0)
    rs_d.relays(1)
    dn_rows(1)
    dn_rows(3)
    rs_d.owns(0)
    rs_d.owns(1)
    dn_rows(0)
    ag_o = Gather(ring, s['bo'], s['gsem'].at[5], s['gr'].at[0], s['gd3'].at[0], s['gsem'].at[8])
    s['bo'][core, chip] = pack(mine(s['e24'][...]) + rs_y.finish())
    ag_o.start()
    for i in range(2):
        for j, p in enumerate(parts(s['bs'][i].reshape(vocab, half))):
            s['sp'][3 * i + j] = p

    hid_own = own(s['hid'][...].astype(F32)).astype(BF)
    for i in range(2):
        acc = jnp.zeros((f_loc, half), F32)
        for j in (2, 1, 0):
            acc = acc + dot(hid_own, s['sp'][3 * i + j], 0, 0)
        if i == 0:
            dw2_ref[:, :half] = acc
        else:
            dw2_ref[:, half:] = acc[:, :rest]

    rs_d.middle(0)
    rs_d.middle(1)
    ag_o.first(1)
    ag_o.first(3)
    ag_o.first(2)
    ag_o.middle(0)
    rs_d.short(2)
    rs_d.short(1)
    rs_d.short(3)
    du_own = parts(own(s['dh'][...].reshape(vocab, f_chip)))
    for i in range(2):
        acc = jnp.zeros((f_loc, half), F32)
        for p in du_own[::-1]:
            acc = acc + dot(p, s['n'][i], 0, 0)
        if i == 0:
            dw1_ref[:, :half] = acc
        else:
            dw1_ref[:, half:] = acc[:, :rest]

    rs_d.short(0)
    ag_o.middle(1)
    ag_o.middle(3)
    ag_o.middle(2)
    s['dnx'][core] = rs_d.finish()
    r_dn = pair(s['dnx'].at[core], s['dnx'].at[core], 5)
    r_dn.start()
    ag_o.last(0)
    ag_o.last(3)
    ag_o.last(1)
    ag_o.last(2)
    pair(s['dnx'].at[1 - core], s['dnx'].at[1 - core], 5).wait_recv()
    inv = inv_rms(s['e24'][...])
    xr = s['e24'][...] * inv
    gd = gain * jnp.concatenate([s['dnx'][0], s['dnx'][1]], axis=1)
    dx = inv * (gd - xr * (jnp.sum(xr * gd, axis=-1, keepdims=True) / width))
    dx = dx + jnp.concatenate([s['bs'][0, chip], s['bs'][1, chip]], axis=1)
    de_ref[...] = jnp.where(core == 0, dx[:rows_e], dx[rows_e:])[:, :width]

    ag_o.finish()
    unpack(s['bo'], o_ref)


    for c in (r_e, r_i, r_w1, r_w2, r_dn):
        c.wait_send()
    for i in range(2):
        @pl.when(core == i)
        def _():
            d_give[i].wait_send()
    for x in (ag_n, rs_s, ag_s, rs_y, rs_d, ag_o):
        x.drain()


def rows_out(ids, o, de, dw1, dw2, out_ref, de_ref, dw1_ref, dw2_ref, buf, sem):
    _, vocab, half = o.shape
    copies = [pltpu.make_async_copy(src, dst, sem.at[i]) for i, (src, dst) in enumerate(
        ((dw1, dw1_ref), (dw2, dw2_ref), (de, de_ref), (buf.at[:half], out_ref.at[:half]), (buf.at[half:], out_ref.at[half:])))]
    for c in copies[:3]:
        c.start()
    mask = hot(ids[...], vocab)
    buf[:half] = dot(o[0], mask, 0, 0).astype(BF)
    copies[3].start()
    buf[half:] = dot(o[1], mask, 0, 0)[:buf.shape[0] - half].astype(BF)
    copies[4].start()
    for c in copies:
        c.wait()


def solution(mesh):
    tok_spec = P(('data', 'tensor'))
    row_spec = P(('data', 'tensor'), None)
    n_tensor = mesh.shape['tensor']
    chips = n_tensor // CORES
    side = math.isqrt(chips)
    assert side == 4 and side * side == chips

    def local_step(token_ids, emb_shard, norm_gain, w_up, w_down, grad_out):
        rows_e, width = emb_shard.shape
        tokens = token_ids.shape[0]
        f_loc = w_up.shape[1]
        f_chip = CORES * f_loc
        half = -(-width // 256) * 128
        rb = CORES * rows_e
        vocab = chips * rb
        vm = pltpu.VMEM
        dma = lambda *shape: pltpu.SemaphoreType.DMA(shape)
        scratch = dict(
            es=vm((2, rows_e, width), BF), gsrc=vm((width,), BF), ids=vm((2, 1, tokens), jnp.int32),
            w1s=vm((2, f_loc, width), BF), w2s=vm((2, f_loc, width), BF), dt=vm((2, half, tokens), BF), dg=vm((half, tokens), BF),
            e24=vm((rb, 2 * half), F32), w1p=vm((2, f_chip, half), BF), w2p=vm((2, f_chip, half), BF),
            bn=vm((2, chips, 2 * rb, half // 2), BF), bo=vm((2, chips, 2 * rb, half // 2), BF),
            bs=vm((2, chips, rb, half), F32), sp=vm((6, vocab, half), BF),
            n=vm((2, vocab, half), BF),
            gs=vm((chips, rb, half), F32), gy=vm((chips, rb, half), F32), gd=vm((chips, rb, half), F32),
            lay=vm((3, 4, rb, half), F32), ra=vm((3, 2, 4, rb, half), F32), rb=vm((3, 3, rb, half), F32),
            r=vm((3, 4, rb, half), F32),
            hid=vm((vocab, f_chip), BF), slope=vm((chips, rb, f_chip), F32), dh=vm((chips, rb, f_chip), F32),
            dnx=vm((2, rb, half), F32),
            lsem=dma(7), psem=dma(6), qsem=dma(6),
            gsem=dma(9), gd3=dma(2, 3), sr=dma(2, 9), gr=dma(2, 15),
        )
        names = list(scratch)

        def body(*refs):
            kernel(side, *refs[:10], dict(zip(names, refs[10:])))

        hbm = pl.BlockSpec(memory_space=pltpu.HBM)
        on_chip = pl.BlockSpec(memory_space=pltpu.VMEM)
        shapes = (
            jax.ShapeDtypeStruct((rows_e, width), F32),
            jax.ShapeDtypeStruct((f_loc, width), F32),
            jax.ShapeDtypeStruct((f_loc, width), F32),
        )
        ids_row = token_ids.reshape(1, tokens)
        done = pl.pallas_call(
            body,
            out_shape=(jax.ShapeDtypeStruct((2, vocab, half), BF),) + shapes,
            in_specs=[hbm] * 6,
            out_specs=(on_chip,) * 4,
            scratch_shapes=list(scratch.values()),
            compiler_params=pltpu.CompilerParams(
                collective_id=0, has_side_effects=True, vmem_limit_bytes=36 * 1024 * 1024),
            name='step',
        )(*(pltpu.with_memory_space_constraint(v, pltpu.HBM) for v in (
            ids_row, emb_shard, norm_gain, w_up.T, w_down, grad_out.T)))
        out_t, d_emb, dw1_t, d_w2 = pl.pallas_call(
            rows_out,
            out_shape=(jax.ShapeDtypeStruct((width, tokens), BF),) + shapes,
            in_specs=[on_chip] * 5,
            out_specs=(hbm,) * 4,
            scratch_shapes=[vm((width, tokens), BF), dma(5)],
            compiler_params=pltpu.CompilerParams(vmem_limit_bytes=16 * 1024 * 1024),
            name='rows_out',
        )(ids_row, *done)
        return out_t.T, d_emb, dw1_t.T, d_w2

    return jax.shard_map(
        local_step,
        mesh=mesh,
        in_specs=(tok_spec, P('tensor', None), P(None), P(None, 'tensor'), P('tensor', None), row_spec),
        out_specs=(row_spec, row_spec, P('data', 'tensor'), row_spec),
        check_vma=False,
    )
```
